512 devices in a mesh: dp: 64 (over x, z, core), tile: 8 (over y).
Axes of the slice: x: 4, y: 8, z: 8, core: 2. Of those that a mesh axis runs over, the one named last changes fastest.
Arguments:
- proposal_boxes: int32 [64, 4, 512], P('dp'), may hold values from 0 to 1344, as said below
- level_plan: int32 [64, 512], P('dp'), may hold values from 0 to 1
- fine_map: bfloat16 [64, 336, 168, 128], P('dp', 'tile'), may hold values from -6 to 6
- coarse_map: bfloat16 [64, 168, 84, 128], P('dp', 'tile'), may hold values from -6 to 6
- first_weight: bfloat16 [6272, 1024], P('tile', 'dp'), may hold values from -0.078125 to 0.078125
- second_weight: bfloat16 [1024, 1024], P('tile', 'dp'), may hold values from -0.1875 to 0.1875
- upstream: bfloat16 [64, 512, 1024], P('dp'), may hold values from -6 to 6
Outputs:
- first_grad: float32 [6272, 1024], P('tile', 'dp')
- second_grad: float32 [1024, 1024], P('tile', 'dp')
The draws below stay inside these ranges and needn't reach their ends.
Inputs may be any that keep to these rules, and one draw needn't show every extreme that they name: `proposal_boxes`: with s = 4 where level_plan is 0 and s = 8 where it is 1: h >= 1, w >= 1, y0 + h <= 1344, x0 + w <= 672, (y0 mod s) + h <= 14 * s and (x0 mod s) + w <= 14 * s. Band b holds the proposals with b * 168 <= y0 < (b + 1) * 168; at most 128 of an image's proposals lie in one band, and in every image some band holds exactly 128.
All inputs are finite; a program needn't handle non-finite values.
Results may differ from the reference program's by a relative error of at most 0.017.
Values may be sent and summed in bfloat16 or wider, within the bound.
No kernel may reach another device: no remote copies, remote signals or barrier semaphores. Data moves between devices by JAX's collectives and lax.ppermute only.
A program may use at most 64 MiB of HBM per device.

```python
import jax
import jax.numpy as jnp
from jax import lax

CH = 128
HIDDEN_SIZE = 1024
FEATS = 6272
WIN = 16
ROWS2 = 42
COLS2 = 168
ROWS3 = 21
COLS3 = 84
PROPS = 512
CAP = 128
IMAGES = 64
BAND_PX = 168
HEIGHT_PX = 1344
WIDTH_PX = 672
N_TILE = 8


def proposal_plan(key):
    base_key = jax.random.fold_in(key, 11)
    key_level, key_busy, key_order, key_top, key_height, key_left, key_width = jax.random.split(base_key, 7)
    grid_shape = (IMAGES, PROPS)
    level_draw = jax.random.randint(key_level, grid_shape, 0, 2)
    busy_band = jax.random.randint(key_busy, (IMAGES, 1), 0, N_TILE)
    slot_index = jnp.arange(PROPS)[None, :]
    other_bands = max(N_TILE - 1, 1)
    spread_band = (busy_band + 1 + jnp.maximum(slot_index - CAP, 0) % other_bands) % N_TILE
    listed_band = jnp.where(slot_index < CAP, busy_band, spread_band)
    shuffles = jax.vmap(lambda order_key: jax.random.permutation(order_key, PROPS))(jax.random.split(key_order, IMAGES))
    owner_band = jnp.take_along_axis(listed_band, shuffles, axis=1)
    stride = jnp.where(level_draw == 0, 4, 8)
    top_pixel = owner_band * BAND_PX + jax.random.randint(key_top, grid_shape, 0, BAND_PX)
    height_most = jnp.minimum(14 * stride - top_pixel % stride, HEIGHT_PX - top_pixel)
    height_draw = jax.random.randint(key_height, grid_shape, jnp.minimum(stride, height_most), height_most + 1)
    left_pixel = jax.random.randint(key_left, grid_shape, 0, WIDTH_PX)
    width_most = jnp.minimum(14 * stride - left_pixel % stride, WIDTH_PX - left_pixel)
    width_draw = jax.random.randint(key_width, grid_shape, jnp.minimum(stride, width_most), width_most + 1)
    box_array = jnp.stack([top_pixel, left_pixel, height_draw, width_draw], axis=1).astype(jnp.int32)
    return (box_array, level_draw.astype(jnp.int32))


def draw_proposal_boxes(key, part):
    return proposal_plan(key)[0]


def draw_level_plan(key, part):
    return proposal_plan(key)[1]


def block_scale(stream_key, shape, shards, low, high):
    gain, own = 1.0, jax.random.fold_in(stream_key, 6)
    for axis_at, shards_of in shards:
        draws = jnp.exp(jax.random.uniform(jax.random.fold_in(own, axis_at), (shards_of,), jnp.float32, low / len(shards), high / len(shards)))
        gain = gain * jnp.repeat(draws, shape[axis_at] // shards_of).reshape([-1 if axis == axis_at else 1 for axis in range(len(shape))])
    return gain


def gaussian(own_key, dims, scale, limit, cuts=(), held_as=jnp.bfloat16):
    entries = jax.random.normal(own_key, dims, jnp.float32) * scale
    if len(cuts) > 0:
        entries = block_scale(own_key, dims, cuts, -0.22, 0.18) * entries
    return jnp.clip(entries, min=-limit, max=limit).astype(held_as)


def setup_inputs(seed: int = 0) -> dict:
    key_of = jax.random.split(jax.random.key(seed), 8)
    proposal_boxes = draw_proposal_boxes(jax.random.fold_in(key_of[7], 71), 0)
    level_plan = draw_level_plan(jax.random.fold_in(key_of[7], 71), 0)
    fine_map = gaussian(key_of[2], (IMAGES, ROWS2 * N_TILE, COLS2, CH), 1.0, 6.0, ((0, 64), (1, 8)))
    coarse_map = gaussian(key_of[3], (IMAGES, ROWS3 * N_TILE, COLS3, CH), 1.0, 6.0, ((0, 64), (1, 8)))
    first_weight = gaussian(key_of[4], (FEATS, HIDDEN_SIZE), FEATS ** -0.5, 0.078125, ((0, 8), (1, 64)))
    second_weight = gaussian(key_of[5], (HIDDEN_SIZE, HIDDEN_SIZE), HIDDEN_SIZE ** -0.5, 0.1875, ((0, 8), (1, 64)))
    upstream = gaussian(key_of[6], (IMAGES, PROPS, HIDDEN_SIZE), 1.0, 6.0, ((0, 64),))
    return {"proposal_boxes": proposal_boxes, "level_plan": level_plan, "fine_map": fine_map, "coarse_map": coarse_map, "first_weight": first_weight, "second_weight": second_weight, "upstream": upstream}


def gelu_parts(hidden):
    factor = 0.7978845608028654
    cubic_term = 0.044715
    inner_term = factor * (hidden + cubic_term * hidden * hidden * hidden)
    tangent = jnp.tanh(inner_term)
    gelu_value = 0.5 * hidden * (1.0 + tangent)
    gelu_slope = 0.5 * (1.0 + tangent) + 0.5 * hidden * (1.0 - tangent * tangent) * factor * (1.0 + 3.0 * cubic_term * hidden * hidden)
    return gelu_value, gelu_slope


def block_size(num_items):
    return 32 if num_items % 32 == 0 else num_items


def axis_weights(begin_px, extent, first_cell, stride):
    stride_float = stride.astype(jnp.float32)[:, None]
    bin_index = jnp.arange(7, dtype=jnp.float32)[None, :]
    sample_pos = begin_px.astype(jnp.float32)[:, None] / stride_float + (bin_index + 0.5) * extent.astype(jnp.float32)[:, None] / (7.0 * stride_float)
    cell_pos = first_cell.astype(jnp.float32)[:, None, None] + jnp.arange(WIN, dtype=jnp.float32)[None, None, :]
    return jnp.maximum(0.0, 1.0 - jnp.abs(sample_pos[:, :, None] - cell_pos))


def crop_block(combined, fields, levels_blk, shift_fine, shift_coarse, limit_fine, limit_coarse, offset):
    top_pixel = fields[0]
    left_pixel = fields[1]
    height = fields[2]
    box_width = fields[3]
    stride = jnp.where(levels_blk == 0, 4, 8).astype(jnp.int32)
    first_row = (top_pixel // stride).astype(jnp.int32)
    first_col = jnp.minimum(left_pixel // stride, jnp.where(levels_blk == 0, limit_fine, limit_coarse) - WIN).astype(jnp.int32)
    start_row = jnp.where(levels_blk == 0, first_row - shift_fine, offset + first_row - shift_coarse).astype(jnp.int32)
    channels = combined.shape[2]
    zero_index = jnp.zeros((), jnp.int32)

    def window(row_start, col_start):
        return lax.dynamic_slice(combined, (row_start.astype(jnp.int32), col_start.astype(jnp.int32), zero_index), (WIN, WIN, channels))

    windows = jax.vmap(window)(start_row, first_col).astype(jnp.float32)
    row_low = lax.optimization_barrier(axis_weights(top_pixel, height, first_row, stride).astype(jnp.bfloat16))
    col_low = lax.optimization_barrier(axis_weights(left_pixel, box_width, first_col, stride).astype(jnp.bfloat16))
    row_weights = row_low.astype(jnp.float32)
    col_weights = col_low.astype(jnp.float32)
    partial_rows = jnp.einsum("bia,baqc->biqc", row_weights, windows, precision=lax.Precision.HIGHEST)
    crop_rows = jnp.einsum("bjq,biqc->bijc", col_weights, partial_rows, precision=lax.Precision.HIGHEST)
    return crop_rows.reshape(crop_rows.shape[0], 49 * channels).astype(jnp.bfloat16)


def image_crops(inputs):
    fields, levels_img, fine_tile, coarse = inputs
    fine_rows, fine_cols, channels = fine_tile.shape
    coarse_cols = coarse.shape[1]
    fine_pad = jnp.pad(fine_tile, ((0, WIN), (0, WIN), (0, 0)))
    coarse_pad = jnp.pad(coarse, ((0, WIN), (0, fine_cols + WIN - coarse_cols), (0, 0)))
    combined = jnp.concatenate([fine_pad, coarse_pad], axis=0)
    num_props = levels_img.shape[0]
    block_len = block_size(num_props)
    grouped_fields = fields.reshape(4, num_props // block_len, block_len).transpose(1, 0, 2)
    grouped_levels = levels_img.reshape(num_props // block_len, block_len)

    def crop_group(pieces):
        part_fields, part_levels = pieces
        return crop_block(combined, part_fields, part_levels, 0, 0, fine_cols + WIN, coarse_cols + WIN, fine_rows + WIN)

    grouped = lax.map(crop_group, (grouped_fields, grouped_levels))
    return grouped.reshape(num_props, 49 * channels)


def reference(proposal_boxes, level_plan, fine_map, coarse_map, first_weight, second_weight, upstream):
    crop_all = lax.map(image_crops, (proposal_boxes, level_plan, fine_map, coarse_map))
    flat_crops = crop_all.reshape(-1, crop_all.shape[2])
    upstream_rows = upstream.reshape(-1, upstream.shape[2])
    hidden = jnp.dot(flat_crops, first_weight, preferred_element_type=jnp.float32)
    gelu_value, gelu_slope = gelu_parts(hidden)
    activated = gelu_value.astype(jnp.bfloat16)
    second_grad = jnp.dot(activated.T, upstream_rows, preferred_element_type=jnp.float32)
    back_grad = jnp.dot(upstream_rows, second_weight.T, preferred_element_type=jnp.float32)
    pre_grad = (back_grad * gelu_slope).astype(jnp.bfloat16)
    first_grad = jnp.dot(flat_crops.T, pre_grad, preferred_element_type=jnp.float32)
    return first_grad, second_grad
```

```python
import jax
import jax.numpy as jnp
from jax import lax
from jax.experimental import pallas as pl
from jax.experimental.pallas import tpu as pltpu
from jax.sharding import Mesh, PartitionSpec as P


REACH = 14
SPAN = 32
GROUP = 8
BF = jnp.bfloat16
F32 = jnp.float32


def gelu_parts(hidden):
    factor = 0.7978845608028654
    cubic_term = 0.044715
    inner_term = factor * (hidden + cubic_term * hidden * hidden * hidden)
    tangent = jnp.tanh(inner_term)
    gelu_value = 0.5 * hidden * (1.0 + tangent)
    gelu_slope = 0.5 * (1.0 + tangent) + 0.5 * hidden * (1.0 - tangent * tangent) * factor * (
        1.0 + 3.0 * cubic_term * hidden * hidden
    )
    return (gelu_value, gelu_slope)


def top_kernel(fine_ref, coarse_ref, fine_top_ref, coarse_top_ref, arrived):
    moves = [
        pltpu.make_async_copy(fine_ref.at[0:REACH], fine_top_ref, arrived.at[0]),
        pltpu.make_async_copy(coarse_ref.at[0:REACH], coarse_top_ref, arrived.at[1]),
    ]
    for move in moves:
        move.start()
    for move in moves:
        move.wait()


def cut_tops(fine, coarse):
    away = pl.BlockSpec(memory_space=pl.ANY)
    return pl.pallas_call(
        top_kernel,
        out_shape=(
            jax.ShapeDtypeStruct((REACH, *fine.shape[1:]), BF),
            jax.ShapeDtypeStruct((REACH, *coarse.shape[1:]), BF),
        ),
        in_specs=[away, away],
        out_specs=(pl.BlockSpec(memory_space=pltpu.VMEM), pl.BlockSpec(memory_space=pltpu.VMEM)),
        scratch_shapes=[pltpu.SemaphoreType.DMA((2,))],
        name="tops",
    )(fine, coarse)


def plan_kernel(band_ref, box_ref, level_ref, slot_ref, ints_ref, reals_ref, *, shape):
    tiles, capacity, fine_rows, coarse_rows, stride = shape
    props = level_ref.shape[1]
    band = band_ref[0]
    top, left, height, width = (box_ref[i : i + 1, :] for i in range(4))
    level = level_ref[...]
    rows_px = stride * fine_rows
    owner = jnp.zeros_like(top)
    for b in range(1, tiles):
        owner = owner + jnp.where(top >= b * rows_px, 1, 0)
    down = (top - owner * rows_px).astype(F32)
    scale = jnp.where(level == 0, 1.0 / stride, 0.5 / stride)
    last = down * scale + 6.5 * height.astype(F32) * (scale / 7.0)
    limit = jnp.where(level == 0, float(fine_rows), float(coarse_rows))
    crosses = jnp.where(last >= limit - 1.01, 1.0, 0.0)
    inside = lax.broadcasted_iota(jnp.int32, (tiles, props), 0) == owner
    late = jnp.where(inside, crosses, 0.0)
    early = jnp.where(inside, 1.0 - crosses, 0.0)
    upto = lax.broadcasted_iota(jnp.int32, (props, props), 0) <= lax.broadcasted_iota(
        jnp.int32, (props, props), 1
    )
    upto = jnp.where(upto, 1.0, 0.0).astype(BF)
    both = jnp.concatenate([early, late], axis=0).astype(BF)
    order = jnp.dot(both, upto, preferred_element_type=F32)
    first = jnp.sum(early, axis=1, keepdims=True)
    every = first + jnp.sum(late, axis=1, keepdims=True)
    rank = early * (order[:tiles] - 1.0) + late * (order[tiles:] + first - 1.0)
    rank = jnp.sum(rank, axis=0, keepdims=True).astype(jnp.int32)
    slot = owner * capacity + rank
    slot_ref[...] = slot
    here = lax.broadcasted_iota(jnp.int32, (capacity, props), 0) + band * capacity == slot
    here = jnp.where(here, 1.0, 0.0).astype(BF)
    fields = jnp.concatenate(
        [
            down,
            (left // 8).astype(F32),
            (left % 8).astype(F32),
            height.astype(F32),
            width.astype(F32),
            level.astype(F32),
            jnp.ones_like(down),
            jnp.zeros_like(down),
        ],
        axis=0,
    ).astype(BF)
    fields = jnp.concatenate([fields, jnp.zeros_like(fields)], axis=0)
    taken = lax.dot_general(fields, here, (((1,), (1,)), ((), ())), preferred_element_type=F32)
    down, left_high, left_low, height, width, level, live = (taken[i : i + 1] for i in range(7))
    scale = jnp.where(level > 0.5, 0.5 / stride, 1.0 / stride)
    step = lax.broadcasted_iota(jnp.int32, (8, capacity), 0).astype(F32) + 0.5
    point = down * scale + step * (height * (scale / 7.0))
    whole = jnp.floor(point)
    near = jnp.maximum(0.0, 1.0 - (point - whole)).astype(BF).astype(F32)
    far = jnp.maximum(0.0, 1.0 - (whole + 1.0 - point)).astype(BF).astype(F32)
    most = jnp.where(level > 0.5, float(coarse_rows), float(fine_rows)) + (REACH - 2.0)
    whole = jnp.clip(whole, 0.0, most) + jnp.where(level > 0.5, fine_rows + float(REACH), 0.0)
    across = (left_high * 8.0 + left_low) * scale
    col = jnp.floor(across * 0.0625) * 16.0
    own = lax.broadcasted_iota(jnp.int32, (tiles, 1), 0) == band
    early_count = jnp.sum(jnp.where(own, first, 0.0), axis=0, keepdims=True)
    every_count = jnp.sum(jnp.where(own, every, 0.0), axis=0, keepdims=True)
    at = lax.broadcasted_iota(jnp.int32, (8, capacity), 0)
    extra = jnp.where(at == 0, col, jnp.where(at == 1, early_count, every_count))
    ints_ref[0:8] = whole.astype(jnp.int32)
    ints_ref[8:16] = extra.astype(jnp.int32)
    reals_ref[0:8] = near * live
    reals_ref[8:16] = far * live
    reals_ref[16:24] = jnp.where(at == 0, across - col, width * (scale / 7.0))


def make_plan(band, boxes, levels, tiles, capacity, fine_rows, coarse_rows, stride):
    smem = pl.BlockSpec(memory_space=pltpu.SMEM)
    vmem = pl.BlockSpec(memory_space=pltpu.VMEM)

    def kernel(*refs):
        plan_kernel(*refs, shape=(tiles, capacity, fine_rows, coarse_rows, stride))

    return pl.pallas_call(
        kernel,
        out_shape=(
            jax.ShapeDtypeStruct(levels.shape, jnp.int32),
            jax.ShapeDtypeStruct((16, capacity), jnp.int32),
            jax.ShapeDtypeStruct((24, capacity), F32),
        ),
        in_specs=[smem, vmem, vmem],
        out_specs=(vmem, vmem, vmem),
        name="plan",
    )(band, boxes, levels)


def fill_maps(maps, fine_ref, coarse_ref, below, arrived):
    fine_rows, fine_cols, channels = fine_ref.shape
    coarse_rows, coarse_cols, _ = coarse_ref.shape
    total, pitch, _ = maps.shape
    base = fine_rows + REACH
    fine_copy = pltpu.make_async_copy(
        fine_ref, maps.at[0:fine_rows, 0:fine_cols, :], arrived.at[0]
    )
    fine_copy.start()
    maps[0:base, fine_cols:pitch, :] = jnp.zeros((base, pitch - fine_cols, channels), BF)
    maps[base:total, :, :] = jnp.zeros((total - base, pitch, channels), BF)
    maps[base : base + coarse_rows, 0:coarse_cols, :] = coarse_ref[...]
    if below is None:
        maps[fine_rows:base, 0:fine_cols, :] = jnp.zeros((REACH, fine_cols, channels), BF)
    else:
        maps[fine_rows:base, 0:fine_cols, :] = below[0][...]
        maps[base + coarse_rows : total, 0:coarse_cols, :] = below[1][...]
    fine_copy.wait()


def fill_cells(bin_ref, cell_ref):
    line = lax.broadcasted_iota(jnp.int32, bin_ref.shape, 0).astype(F32)
    lane = lax.broadcasted_iota(jnp.int32, bin_ref.shape, 1).astype(F32)
    row = jnp.floor((line + 0.5) * (1.0 / 7.0))
    piece = jnp.floor((lane + 0.5) * (1.0 / SPAN))
    bin_ref[...] = line - 7.0 * row + 0.5
    cell_ref[...] = jnp.where(row == piece, lane - SPAN * piece, 1.0e6)


def crop_group(step, ints_ref, reals_ref, bin_ref, cell_ref, maps, parts, crops):
    channels = maps.shape[2]
    bins = parts.shape[1]
    first = step * GROUP
    for g in range(GROUP):
        slot = first + g
        col = pl.multiple_of(ints_ref[8, slot], 16)
        lines = []
        for i in range(7):
            row = ints_ref[i, slot]
            upper = maps[row, pl.ds(col, SPAN), :].astype(F32)
            lower = maps[row + 1, pl.ds(col, SPAN), :].astype(F32)
            lines.append((reals_ref[i, slot] * upper + reals_ref[8 + i, slot] * lower).astype(BF))
        lines.append(jnp.zeros((SPAN, channels), BF))
        stacked = jnp.concatenate(lines, axis=0)
        away = (reals_ref[16, slot] + bin_ref[...] * reals_ref[17, slot]) - cell_ref[...]
        mix = jnp.maximum(0.0, 1.0 - jnp.abs(away)).astype(BF)
        parts[g] = jnp.dot(mix, stacked, preferred_element_type=F32)
    flat = parts.reshape(GROUP * bins, channels)
    start = pl.multiple_of(first, GROUP)
    for m in range(49):
        crops[m, pl.ds(start, GROUP), :] = flat[pl.ds(m, GROUP, stride=bins), :]


def inner_kernel(ints_ref, reals_ref, fine_ref, coarse_ref, crops_ref, maps, parts, bin_ref,
                 cell_ref, arrived):
    fill_cells(bin_ref, cell_ref)
    fill_maps(maps, fine_ref, coarse_ref, None, arrived)

    def body(step, carry):
        crop_group(step, ints_ref, reals_ref, bin_ref, cell_ref, maps, parts, crops_ref)
        return carry

    lax.fori_loop(0, crops_ref.shape[1] // GROUP, body, 0)


def edge_kernel(ints_ref, reals_ref, fine_ref, coarse_ref, fine_below_ref, coarse_below_ref,
                inner_ref, band_ref, *rest):
    *outs, maps, parts, bin_ref, cell_ref, arrived, crops, early, flipped = rest
    channels = fine_ref.shape[2]
    early_copy = pltpu.make_async_copy(inner_ref, early, arrived.at[1])
    early_copy.start()
    fill_cells(bin_ref, cell_ref)
    fill_maps(maps, fine_ref, coarse_ref, (fine_below_ref, coarse_below_ref), arrived)
    low = ints_ref[9, 0] // GROUP
    high = (ints_ref[10, 0] + (GROUP - 1)) // GROUP

    def body(step, carry):
        crop_group(step, ints_ref, reals_ref, bin_ref, cell_ref, maps, parts, crops)
        return carry

    lax.fori_loop(low, high, body, 0)
    early_copy.wait()
    at = lax.broadcasted_iota(jnp.int32, (crops.shape[1], channels), 0)
    redone = (at >= low * GROUP) & (at < high * GROUP)
    for m in range(49):
        block = jnp.where(redone, crops[m], early[m])
        flipped[m * channels : (m + 1) * channels, :] = block.T.astype(BF)
    share = outs[0].shape[0]
    for k, out in enumerate(outs):
        block = (band_ref[0] + k) % len(outs)
        out[...] = flipped[pl.ds(pl.multiple_of(block * share, 16), share), :]


def make_crops(ints, reals, fine, coarse, band, tiles):
    capacity = ints.shape[1]
    channels = fine.shape[2]
    total = fine.shape[0] + coarse.shape[0] + 2 * REACH
    smem = pl.BlockSpec(memory_space=pltpu.SMEM)
    vmem = pl.BlockSpec(memory_space=pltpu.VMEM)
    away = pl.BlockSpec(memory_space=pl.ANY)
    common = [
        pltpu.VMEM((total, 192, channels), BF),
        pltpu.VMEM((GROUP, 56, channels), F32),
        pltpu.VMEM((56, 8 * SPAN), F32),
        pltpu.VMEM((56, 8 * SPAN), F32),
        pltpu.SemaphoreType.DMA((2,)),
    ]
    every = jax.ShapeDtypeStruct((49, capacity, channels), F32)
    params = pltpu.CompilerParams(vmem_limit_bytes=48 << 20)
    inner = pl.pallas_call(
        inner_kernel,
        out_shape=every,
        in_specs=[smem, smem, away, vmem],
        out_specs=vmem,
        scratch_shapes=common,
        compiler_params=params,
        name="inner",
    )
    edge = pl.pallas_call(
        edge_kernel,
        out_shape=[jax.ShapeDtypeStruct((49 * channels // tiles, capacity), BF)] * tiles,
        in_specs=[smem, smem, away, vmem, vmem, vmem, away, smem],
        out_specs=[vmem] * tiles,
        scratch_shapes=common
        + [
            pltpu.VMEM(every.shape, F32),
            pltpu.VMEM(every.shape, F32),
            pltpu.VMEM((49 * channels, capacity), BF),
        ],
        compiler_params=params,
        name="edge",
    )
    early = inner(ints, reals, fine, coarse)
    return early, lambda early, fine_below, coarse_below: edge(
        ints, reals, fine, coarse, fine_below, coarse_below, early, band
    )


def hidden_kernel(band_ref, slot_ref, weight_ref, *rest):
    *recvs, feats_ref, out_ref, joined, pick, arrived = rest
    count = len(recvs)
    share, capacity = recvs[0].shape
    props = slot_ref.shape[1]
    slots = slot_ref[...]
    moves = [
        pltpu.make_async_copy(
            recv, joined.at[:, k * capacity : (k + 1) * capacity], arrived.at[k]
        )
        for k, recv in enumerate(recvs)
    ]
    for move in moves:
        move.start()
    for k in range(count):
        source = (band_ref[0] + count - k) % count
        at = lax.broadcasted_iota(jnp.int32, (capacity, props), 0) + source * capacity
        pick[k * capacity : (k + 1) * capacity, :] = jnp.where(at == slots, 1.0, 0.0).astype(BF)
    for move in moves:
        move.wait()
    feats_ref[...] = jnp.dot(joined[...], pick[...], preferred_element_type=F32).astype(BF)
    skip = weight_ref.shape[1] - share
    out_ref[...] = jnp.dot(
        weight_ref[:, skip:], feats_ref[...], preferred_element_type=F32
    ).astype(BF)


def make_hidden(band, slot_id, weight, recvs):
    share, capacity = recvs[0].shape
    props = slot_id.shape[1]
    smem = pl.BlockSpec(memory_space=pltpu.SMEM)
    vmem = pl.BlockSpec(memory_space=pltpu.VMEM)
    return pl.pallas_call(
        hidden_kernel,
        out_shape=(
            jax.ShapeDtypeStruct((share, props), BF),
            jax.ShapeDtypeStruct((weight.shape[0], props), BF),
        ),
        in_specs=[smem, vmem, vmem] + [pl.BlockSpec(memory_space=pl.ANY)] * len(recvs),
        out_specs=(vmem, vmem),
        scratch_shapes=[
            pltpu.VMEM((share, len(recvs) * capacity), BF),
            pltpu.VMEM((len(recvs) * capacity, props), BF),
            pltpu.SemaphoreType.DMA((len(recvs),)),
        ],
        compiler_params=pltpu.CompilerParams(vmem_limit_bytes=48 << 20),
        name="hidden",
    )(band, slot_id, weight, *recvs)


def act_kernel(pieces_ref, back_ref, act_ref, pre_ref):
    hidden = jnp.sum(pieces_ref[...].astype(F32), axis=0)
    value, slope = gelu_parts(hidden)
    act_ref[...] = value.astype(BF)
    pre = (back_ref[...] * slope).astype(BF)
    for t in range(pre_ref.shape[0]):
        pre_ref[t] = pre


def make_act(pieces, back):
    vmem = pl.BlockSpec(memory_space=pltpu.VMEM)
    return pl.pallas_call(
        act_kernel,
        out_shape=(
            jax.ShapeDtypeStruct(pieces.shape[1:], BF),
            jax.ShapeDtypeStruct(pieces.shape, BF),
        ),
        in_specs=[vmem, vmem],
        out_specs=(vmem, vmem),
        name="act",
    )(pieces, back)


def grads_kernel(core_ref, pre_ref, feats_ref, second_ref, keep_ref, give_ref):
    rows = 256
    unit = keep_ref.shape[1]
    lead = second_ref.shape[1]
    mine = core_ref[0] == 0

    def block(step, carry):
        start = pl.multiple_of(step * rows, rows)
        first = lax.dot_general(
            pre_ref[pl.ds(start, rows), :], feats_ref[...], (((1,), (1,)), ((), ())),
            preferred_element_type=F32,
        ).astype(BF)
        second = second_ref[pl.ds(start, rows), :]
        for n in range(rows // (2 * unit)):
            at = step * (rows // (2 * unit)) + n
            for part, low, high in ((first, lead, keep_ref.shape[2]), (second, 0, lead)):
                even = part[2 * n * unit : (2 * n + 1) * unit]
                odd = part[(2 * n + 1) * unit : (2 * n + 2) * unit]
                keep_ref[at, :, low:high] = jnp.where(mine, even, odd)
                give_ref[at, :, low:high] = jnp.where(mine, odd, even)
        return carry

    lax.fori_loop(0, pre_ref.shape[0] // rows, block, 0)


def make_grads(core, pre, feats, second, unit):
    width = feats.shape[0] + second.shape[1]
    smem = pl.BlockSpec(memory_space=pltpu.SMEM)
    vmem = pl.BlockSpec(memory_space=pltpu.VMEM)
    half = jax.ShapeDtypeStruct((pre.shape[0] // (2 * unit), unit, width), BF)
    return pl.pallas_call(
        grads_kernel,
        out_shape=(half, half),
        in_specs=[smem] + [vmem] * 3,
        out_specs=(vmem, vmem),
        compiler_params=pltpu.CompilerParams(vmem_limit_bytes=48 << 20),
        name="grads",
    )(core, pre, feats, second)


def spread(shard, axis, count):
    copies = jnp.broadcast_to(shard[None], (count, *shard.shape))
    return lax.all_to_all(copies, axis, split_axis=0, concat_axis=0, tiled=True)


def swapped(parts, axis):
    return lax.all_to_all(parts, axis, split_axis=0, concat_axis=0, tiled=True)


def per_device(sizes, proposal_boxes, level_plan, fine_map, coarse_map, first_weight,
               second_weight, upstream):
    nx, nz, nc, tile_count = sizes
    dp = ("x", "z", "core")
    dp_count = nx * nz * nc
    band = lax.axis_index("tile")
    fine = fine_map[0]
    coarse = coarse_map[0]
    up = [(i + 1, i) for i in range(tile_count - 1)]
    fine_top, coarse_top = cut_tops(fine, coarse)
    fine_below = lax.ppermute(fine_top, "tile", up)
    coarse_below = lax.ppermute(coarse_top, "tile", up)
    mine = lax.axis_index("core")
    band_at = band[None].astype(jnp.int32)
    num_props = level_plan.shape[1]
    capacity = max(num_props // 4, num_props // tile_count)
    unit = first_weight.shape[1]
    lead = second_weight.shape[0]
    upstream_rows = upstream[0]

    slot_id, ints, reals = make_plan(
        band_at, proposal_boxes[0], level_plan, tile_count, capacity, fine.shape[0],
        coarse.shape[0], 4,
    )
    early, edge = make_crops(ints, reals, fine, coarse, band_at, tile_count)
    shard = jnp.concatenate([second_weight.T, first_weight.T], axis=1)
    shard, early = lax.optimization_barrier((shard, early))
    weights = spread(shard, dp, dp_count).reshape(-1, shard.shape[1])
    crops = edge(early, fine_below, coarse_below)
    recvs = {0: crops[0]}
    for k in range(1, tile_count):
        route = [(i, (i + k) % tile_count) for i in range(tile_count)]
        recvs[k] = lax.ppermute(crops[k], "tile", route)
    weights, recvs[0] = lax.optimization_barrier((weights, recvs[0]))
    recvs = [recvs[k] for k in range(tile_count)]
    back_grad = lax.dot_general(
        weights[:, :lead], upstream_rows, (((0,), (1,)), ((), ())), preferred_element_type=F32
    )
    back_grad, weights = lax.optimization_barrier((back_grad, weights))
    feats, partial_hidden = make_hidden(band_at, slot_id, weights, recvs)
    pieces = swapped(partial_hidden.reshape(tile_count, -1, num_props), "tile")
    activated, copies = make_act(pieces, back_grad)
    pre_grad = swapped(copies, "tile").reshape(-1, num_props)
    second = lax.dot_general(
        upstream_rows, activated, (((0,), (1,)), ((), ())), preferred_element_type=F32
    ).astype(BF)
    core_at = mine[None].astype(jnp.int32)
    keep, give = make_grads(core_at, pre_grad, feats, second, unit)
    got = lax.ppermute(give, "core", [(0, 1), (1, 0)])
    both = (keep.astype(F32) + got.astype(F32)).astype(BF).reshape(nx, nz, unit, -1)
    both = swapped(both, "x").astype(F32).sum(axis=0).astype(BF)
    total = swapped(both, "z").astype(F32).sum(axis=0)
    return (total[:, lead:].T, total[:, :lead].T)


def solution(mesh):
    tile_count = mesh.shape["tile"]
    sizes = (4, mesh.shape["dp"] // 8, 2, tile_count)
    split = Mesh(mesh.devices.reshape(sizes), ("x", "z", "core", "tile"))
    dp = ("x", "z", "core")
    placed = (
        P(dp, None, None),
        P(dp, None),
        P(dp, "tile", None, None),
        P(dp, "tile", None, None),
        P("tile", dp),
        P("tile", dp),
        P(dp, None, None),
    )

    def step(*args):
        return per_device(sizes, *args)

    return jax.shard_map(
        step,
        mesh=split,
        in_specs=placed,
        out_specs=(P("tile", dp), P("tile", dp)),
        check_vma=False,
    )
```

```python
import jax
import jax.numpy as jnp
from jax import lax
from jax.experimental import pallas as pl
from jax.experimental.pallas import tpu as pltpu
from jax.sharding import Mesh, PartitionSpec as P


REACH = 14
SPAN = 32
GROUP = 8
TURNS = (4, 7, 1, 6, 2, 5, 3)
BF = jnp.bfloat16
F32 = jnp.float32


def gelu_parts(hidden):
    factor = 0.7978845608028654
    cubic_term = 0.044715
    inner_term = factor * (hidden + cubic_term * hidden * hidden * hidden)
    tangent = jnp.tanh(inner_term)
    gelu_value = 0.5 * hidden * (1.0 + tangent)
    gelu_slope = 0.5 * (1.0 + tangent) + 0.5 * hidden * (1.0 - tangent * tangent) * factor * (
        1.0 + 3.0 * cubic_term * hidden * hidden
    )
    return (gelu_value, gelu_slope)


def top_kernel(fine_ref, coarse_ref, fine_top_ref, coarse_top_ref, arrived):
    moves = [
        pltpu.make_async_copy(fine_ref.at[0:REACH], fine_top_ref, arrived.at[0]),
        pltpu.make_async_copy(coarse_ref.at[0:REACH], coarse_top_ref, arrived.at[1]),
    ]
    for move in moves:
        move.start()
    for move in moves:
        move.wait()


def cut_tops(fine, coarse):
    away = pl.BlockSpec(memory_space=pltpu.HBM)
    return pl.pallas_call(
        top_kernel,
        out_shape=(
            jax.ShapeDtypeStruct((REACH, *fine.shape[1:]), BF),
            jax.ShapeDtypeStruct((REACH, *coarse.shape[1:]), BF),
        ),
        in_specs=[away, away],
        out_specs=(pl.BlockSpec(memory_space=pltpu.VMEM), pl.BlockSpec(memory_space=pltpu.VMEM)),
        scratch_shapes=[pltpu.SemaphoreType.DMA((2,))],
        compiler_params=pltpu.CompilerParams(vmem_limit_bytes=60 << 20),
        name="tops",
    )(fine, coarse)


def copies_kernel(first_ref, second_ref, out_ref):
    lead = second_ref.shape[1]
    first = first_ref[...]
    second = second_ref[...]

    def body(i, carry):
        out_ref[i, :, 0:lead] = second
        out_ref[i, :, lead:] = first
        return carry

    lax.fori_loop(0, out_ref.shape[0], body, 0)


def make_copies(first, second, count):
    vmem = pl.BlockSpec(memory_space=pltpu.VMEM)
    width = first.shape[1] + second.shape[1]
    return pl.pallas_call(
        copies_kernel,
        out_shape=jax.ShapeDtypeStruct((count, first.shape[0], width), BF),
        in_specs=[vmem, vmem],
        out_specs=vmem,
        compiler_params=pltpu.CompilerParams(vmem_limit_bytes=8 << 20),
        name="copies",
    )(first, second)


def plan_kernel(band_ref, box_ref, level_ref, slot_ref, ints_ref, reals_ref, *, shape):
    tiles, capacity, fine_rows, coarse_rows, stride = shape
    props = level_ref.shape[1]
    band = band_ref[0]
    top, left, height, width = (box_ref[i : i + 1, :] for i in range(4))
    level = level_ref[...]
    rows_px = stride * fine_rows
    owner = jnp.zeros_like(top)
    for b in range(1, tiles):
        owner = owner + jnp.where(top >= b * rows_px, 1, 0)
    down = (top - owner * rows_px).astype(F32)
    scale = jnp.where(level == 0, 1.0 / stride, 0.5 / stride)
    last = down * scale + 6.5 * height.astype(F32) * (scale / 7.0)
    limit = jnp.where(level == 0, float(fine_rows), float(coarse_rows))
    crosses = jnp.where(last >= limit - 1.01, 1.0, 0.0)
    inside = lax.broadcasted_iota(jnp.int32, (tiles, props), 0) == owner
    late = jnp.where(inside, crosses, 0.0)
    early = jnp.where(inside, 1.0 - crosses, 0.0)
    upto = lax.broadcasted_iota(jnp.int32, (props, props), 0) <= lax.broadcasted_iota(
        jnp.int32, (props, props), 1
    )
    upto = jnp.where(upto, 1.0, 0.0).astype(BF)
    both = jnp.concatenate([early, late], axis=0).astype(BF)
    order = jnp.dot(both, upto, preferred_element_type=F32)
    first = jnp.sum(early, axis=1, keepdims=True)
    every = first + jnp.sum(late, axis=1, keepdims=True)
    rank = early * (order[:tiles] - 1.0) + late * (order[tiles:] + first - 1.0)
    rank = jnp.sum(rank, axis=0, keepdims=True).astype(jnp.int32)
    slot = owner * capacity + rank
    slot_ref[...] = slot
    here = lax.broadcasted_iota(jnp.int32, (capacity, props), 0) + band * capacity == slot
    here = jnp.where(here, 1.0, 0.0).astype(BF)
    fields = jnp.concatenate(
        [
            down,
            (left // 8).astype(F32),
            (left % 8).astype(F32),
            height.astype(F32),
            width.astype(F32),
            level.astype(F32),
            jnp.ones_like(down),
            jnp.zeros_like(down),
        ],
        axis=0,
    ).astype(BF)
    fields = jnp.concatenate([fields, jnp.zeros_like(fields)], axis=0)
    taken = lax.dot_general(fields, here, (((1,), (1,)), ((), ())), preferred_element_type=F32)
    down, left_high, left_low, height, width, level, live = (taken[i : i + 1] for i in range(7))
    scale = jnp.where(level > 0.5, 0.5 / stride, 1.0 / stride)
    step = lax.broadcasted_iota(jnp.int32, (8, capacity), 0).astype(F32) + 0.5
    point = down * scale + step * (height * (scale / 7.0))
    whole = jnp.floor(point)
    near = jnp.maximum(0.0, 1.0 - (point - whole)).astype(BF).astype(F32)
    far = jnp.maximum(0.0, 1.0 - (whole + 1.0 - point)).astype(BF).astype(F32)
    most = jnp.where(level > 0.5, float(coarse_rows), float(fine_rows)) + (REACH - 2.0)
    whole = jnp.clip(whole, 0.0, most) + jnp.where(level > 0.5, fine_rows + float(REACH), 0.0)
    across = (left_high * 8.0 + left_low) * scale
    col = jnp.floor(across * 0.0625) * 16.0
    own = lax.broadcasted_iota(jnp.int32, (tiles, 1), 0) == band
    early_count = jnp.sum(jnp.where(own, first, 0.0), axis=0, keepdims=True)
    every_count = jnp.sum(jnp.where(own, every, 0.0), axis=0, keepdims=True)
    at = lax.broadcasted_iota(jnp.int32, (8, capacity), 0)
    extra = jnp.where(at == 0, col, jnp.where(at == 1, early_count, every_count))
    ints_ref[0:8] = whole.astype(jnp.int32)
    ints_ref[8:16] = extra.astype(jnp.int32)
    reals_ref[0:8] = near * live
    reals_ref[8:16] = far * live
    reals_ref[16:24] = jnp.where(at == 0, across - col, width * (scale / 7.0))


def make_plan(band, boxes, levels, tiles, capacity, fine_rows, coarse_rows, stride):
    smem = pl.BlockSpec(memory_space=pltpu.SMEM)
    vmem = pl.BlockSpec(memory_space=pltpu.VMEM)

    def kernel(*refs):
        plan_kernel(*refs, shape=(tiles, capacity, fine_rows, coarse_rows, stride))

    return pl.pallas_call(
        kernel,
        out_shape=(
            jax.ShapeDtypeStruct(levels.shape, jnp.int32),
            jax.ShapeDtypeStruct((16, capacity), jnp.int32),
            jax.ShapeDtypeStruct((24, capacity), F32),
        ),
        in_specs=[smem, vmem, vmem],
        out_specs=(vmem, vmem, vmem),
        compiler_params=pltpu.CompilerParams(vmem_limit_bytes=8 << 20),
        name="plan",
    )(band, boxes, levels)


def fill_maps(maps, fine_ref, coarse_ref, below, arrived):
    fine_rows, fine_cols, channels = fine_ref.shape
    coarse_rows, coarse_cols, _ = coarse_ref.shape
    total, pitch, _ = maps.shape
    base = fine_rows + REACH
    fine_copy = pltpu.make_async_copy(
        fine_ref, maps.at[0:fine_rows, 0:fine_cols, :], arrived.at[0]
    )
    fine_copy.start()
    maps[0:base, fine_cols:pitch, :] = jnp.zeros((base, pitch - fine_cols, channels), BF)
    maps[base:total, :, :] = jnp.zeros((total - base, pitch, channels), BF)
    maps[base : base + coarse_rows, 0:coarse_cols, :] = coarse_ref[...]
    if below is None:
        maps[fine_rows:base, 0:fine_cols, :] = jnp.zeros((REACH, fine_cols, channels), BF)
    else:
        maps[fine_rows:base, 0:fine_cols, :] = below[0][...]
        maps[base + coarse_rows : total, 0:coarse_cols, :] = below[1][...]
    fine_copy.wait()


def fill_cells(bin_ref, cell_ref):
    line = lax.broadcasted_iota(jnp.int32, bin_ref.shape, 0)
    lane = lax.broadcasted_iota(jnp.int32, bin_ref.shape, 1)
    bin_ref[...] = line.astype(F32) + 0.5
    cell_ref[...] = (lane % SPAN).astype(F32)


def crop_group(step, ints_ref, reals_ref, bin_ref, cell_ref, maps, parts, crops):
    channels = maps.shape[2]
    bins = parts.shape[1]
    first = step * GROUP
    for g in range(GROUP):
        slot = first + g
        col = pl.multiple_of(ints_ref[8, slot], 16)
        lines = []
        for i in range(7):
            row = ints_ref[i, slot]
            upper = maps[row, pl.ds(col, SPAN), :]
            lower = maps[row + 1, pl.ds(col, SPAN), :]
            near = jnp.full(upper.shape, reals_ref[i, slot], F32).astype(BF)
            far = jnp.full(upper.shape, reals_ref[8 + i, slot], F32).astype(BF)
            lines.append(near * upper + far * lower)
        lines.append(jnp.zeros((SPAN, channels), BF))
        stacked = jnp.concatenate(lines, axis=0)
        away = (reals_ref[16, slot] + bin_ref[...] * reals_ref[17, slot]) - cell_ref[...]
        line = jnp.maximum(0.0, 1.0 - jnp.abs(away))
        piece = lax.broadcasted_iota(jnp.int32, line.shape, 1) // SPAN
        mix = [jnp.where(piece == i, line, 0.0) for i in range(7)]
        mix = jnp.concatenate(mix, axis=0).astype(BF)
        parts[g] = jnp.dot(mix, stacked, preferred_element_type=F32)
    flat = parts.reshape(GROUP * bins, channels)
    start = pl.multiple_of(first, GROUP)
    for m in range(49):
        at = m // 7 * 8 + m % 7
        crops[m, pl.ds(start, GROUP), :] = flat[pl.ds(at, GROUP, stride=bins), :]


def inner_kernel(ints_ref, reals_ref, fine_ref, coarse_ref, crops_ref, maps, parts, bin_ref,
                 cell_ref, arrived):
    fill_cells(bin_ref, cell_ref)
    fill_maps(maps, fine_ref, coarse_ref, None, arrived)

    def body(step, carry):
        crop_group(step, ints_ref, reals_ref, bin_ref, cell_ref, maps, parts, crops_ref)
        return carry

    lax.fori_loop(0, crops_ref.shape[1] // GROUP, body, 0)


def edge_kernel(ints_ref, reals_ref, fine_ref, coarse_ref, fine_below_ref, coarse_below_ref,
                inner_ref, band_ref, *rest):
    *outs, maps, parts, bin_ref, cell_ref, arrived, crops, early, flipped = rest
    channels = fine_ref.shape[2]
    early_copy = pltpu.make_async_copy(inner_ref, early, arrived.at[1])
    early_copy.start()
    fill_cells(bin_ref, cell_ref)
    fill_maps(maps, fine_ref, coarse_ref, (fine_below_ref, coarse_below_ref), arrived)
    low = ints_ref[9, 0] // GROUP
    high = (ints_ref[10, 0] + (GROUP - 1)) // GROUP

    def body(step, carry):
        crop_group(step, ints_ref, reals_ref, bin_ref, cell_ref, maps, parts, crops)
        return carry

    lax.fori_loop(low, high, body, 0)
    early_copy.wait()
    at = lax.broadcasted_iota(jnp.int32, (crops.shape[1], channels), 0)
    redone = (at >= low * GROUP) & (at < high * GROUP)
    for m in range(49):
        block = jnp.where(redone, crops[m], early[m])
        flipped[m * channels : (m + 1) * channels, :] = block.T.astype(BF)
    share = outs[0].shape[0]
    for k, out in enumerate(outs):
        block = (band_ref[0] + k) % len(outs)
        out[...] = flipped[pl.ds(pl.multiple_of(block * share, 16), share), :]


def make_crops(ints, reals, fine, coarse, band, tiles):
    capacity = ints.shape[1]
    channels = fine.shape[2]
    total = fine.shape[0] + coarse.shape[0] + 2 * REACH
    smem = pl.BlockSpec(memory_space=pltpu.SMEM)
    vmem = pl.BlockSpec(memory_space=pltpu.VMEM)
    away = pl.BlockSpec(memory_space=pltpu.HBM)
    common = [
        pltpu.VMEM((total, 192, channels), BF),
        pltpu.VMEM((GROUP, 56, channels), F32),
        pltpu.VMEM((8, 8 * SPAN), F32),
        pltpu.VMEM((8, 8 * SPAN), F32),
        pltpu.SemaphoreType.DMA((2,)),
    ]
    every = jax.ShapeDtypeStruct((49, capacity, channels), F32)
    params = pltpu.CompilerParams(vmem_limit_bytes=24 << 20)
    inner = pl.pallas_call(
        inner_kernel,
        out_shape=every,
        in_specs=[smem, smem, away, vmem],
        out_specs=vmem,
        scratch_shapes=common,
        compiler_params=params,
        name="inner",
    )
    edge = pl.pallas_call(
        edge_kernel,
        out_shape=[jax.ShapeDtypeStruct((49 * channels // tiles, capacity), BF)] * tiles,
        in_specs=[smem, smem, away, vmem, vmem, vmem, away, smem],
        out_specs=[vmem] * tiles,
        scratch_shapes=common
        + [
            pltpu.VMEM(every.shape, F32),
            pltpu.VMEM(every.shape, F32),
            pltpu.VMEM((49 * channels, capacity), BF),
        ],
        compiler_params=params,
        name="edge",
    )
    early = inner(ints, reals, fine, coarse)
    return early, lambda early, fine_below, coarse_below: edge(
        ints, reals, fine, coarse, fine_below, coarse_below, early, band
    )


def pick_rows(turns, band_ref, slot_ref, recvs, joined, pick, arrived):
    count, capacity = band_ref[1], recvs[0].shape[1]
    slots = slot_ref[...]
    moves = [
        pltpu.make_async_copy(
            recv, joined.at[:, k * capacity : (k + 1) * capacity], arrived.at[k]
        )
        for k, recv in enumerate(recvs)
    ]
    for move in moves:
        move.start()
    for k, turn in enumerate(turns):
        source = (band_ref[0] + count - turn) % count
        at = lax.broadcasted_iota(jnp.int32, (capacity, slots.shape[1]), 0) + source * capacity
        pick[k * capacity : (k + 1) * capacity, :] = jnp.where(at == slots, 1.0, 0.0).astype(BF)
    for move in moves:
        move.wait()
    return jnp.dot(joined[...], pick[...], preferred_element_type=F32)


def make_gather(band, slot_id, recvs, turns):
    share, capacity = recvs[0].shape
    props = slot_id.shape[1]
    count = len(recvs)
    smem = pl.BlockSpec(memory_space=pltpu.SMEM)
    vmem = pl.BlockSpec(memory_space=pltpu.VMEM)

    def gather_kernel(band_ref, slot_ref, *rest):
        *pieces, out_ref, joined, pick, arrived = rest
        out_ref[...] = pick_rows(turns, band_ref, slot_ref, pieces, joined, pick, arrived).astype(BF)

    return pl.pallas_call(
        gather_kernel,
        out_shape=jax.ShapeDtypeStruct((share, props), BF),
        in_specs=[smem, vmem] + [pl.BlockSpec(memory_space=pl.ANY)] * count,
        out_specs=vmem,
        scratch_shapes=[
            pltpu.VMEM((share, count * capacity), BF),
            pltpu.VMEM((count * capacity, props), BF),
            pltpu.SemaphoreType.DMA((count,)),
        ],
        compiler_params=pltpu.CompilerParams(vmem_limit_bytes=16 << 20),
        name="gather",
    )(band, slot_id, *recvs)


def make_hidden(band, slot_id, weight, begun, recvs, turns):
    share, capacity = recvs[0].shape
    props = slot_id.shape[1]
    count = len(recvs)
    smem = pl.BlockSpec(memory_space=pltpu.SMEM)
    vmem = pl.BlockSpec(memory_space=pltpu.VMEM)

    def hidden_kernel(band_ref, slot_ref, weight_ref, begun_ref, *rest):
        *pieces, feats_ref, out_ref, joined, pick, arrived = rest
        late = pick_rows(turns, band_ref, slot_ref, pieces, joined, pick, arrived)
        feats_ref[...] = begun_ref[...] + late.astype(BF)
        skip = weight_ref.shape[1] - share
        out_ref[...] = jnp.dot(
            weight_ref[:, skip:], feats_ref[...], preferred_element_type=F32
        ).astype(BF)

    return pl.pallas_call(
        hidden_kernel,
        out_shape=(
            jax.ShapeDtypeStruct((share, props), BF),
            jax.ShapeDtypeStruct((weight.shape[0], props), BF),
        ),
        in_specs=[smem, vmem, vmem, vmem] + [pl.BlockSpec(memory_space=pl.ANY)] * count,
        out_specs=(vmem, vmem),
        scratch_shapes=[
            pltpu.VMEM((share, count * capacity), BF),
            pltpu.VMEM((count * capacity, props), BF),
            pltpu.SemaphoreType.DMA((count,)),
        ],
        compiler_params=pltpu.CompilerParams(vmem_limit_bytes=24 << 20),
        name="hidden",
    )(band, slot_id, weight, begun, *recvs)


def act_kernel(pieces_ref, back_ref, act_ref, pre_ref):
    hidden = jnp.sum(pieces_ref[...].astype(F32), axis=0)
    value, slope = gelu_parts(hidden)
    act_ref[...] = value.astype(BF)
    pre = (back_ref[...] * slope).astype(BF)
    for t in range(pre_ref.shape[0]):
        pre_ref[t] = pre


def make_act(pieces, back):
    vmem = pl.BlockSpec(memory_space=pltpu.VMEM)
    return pl.pallas_call(
        act_kernel,
        out_shape=(
            jax.ShapeDtypeStruct(pieces.shape[1:], BF),
            jax.ShapeDtypeStruct(pieces.shape, BF),
        ),
        in_specs=[vmem, vmem],
        out_specs=(vmem, vmem),
        compiler_params=pltpu.CompilerParams(vmem_limit_bytes=8 << 20),
        name="act",
    )(pieces, back)


def grads_kernel(core_ref, pre_ref, feats_ref, second_ref, keep_ref, give_ref):
    rows = 256
    unit = keep_ref.shape[1]
    lead = second_ref.shape[1]
    mine = core_ref[0] == 0

    def block(step, carry):
        start = pl.multiple_of(step * rows, rows)
        first = lax.dot_general(
            pre_ref[pl.ds(start, rows), :], feats_ref[...], (((1,), (1,)), ((), ())),
            preferred_element_type=F32,
        ).astype(BF)
        second = second_ref[pl.ds(start, rows), :]
        for n in range(rows // (2 * unit)):
            at = step * (rows // (2 * unit)) + n
            for part, low, high in ((first, lead, keep_ref.shape[2]), (second, 0, lead)):
                even = part[2 * n * unit : (2 * n + 1) * unit]
                odd = part[(2 * n + 1) * unit : (2 * n + 2) * unit]
                keep_ref[at, :, low:high] = jnp.where(mine, even, odd)
                give_ref[at, :, low:high] = jnp.where(mine, odd, even)
        return carry

    lax.fori_loop(0, pre_ref.shape[0] // rows, block, 0)


def make_grads(core, pre, feats, second, unit):
    width = feats.shape[0] + second.shape[1]
    smem = pl.BlockSpec(memory_space=pltpu.SMEM)
    vmem = pl.BlockSpec(memory_space=pltpu.VMEM)
    half = jax.ShapeDtypeStruct((pre.shape[0] // (2 * unit), unit, width), BF)
    return pl.pallas_call(
        grads_kernel,
        out_shape=(half, half),
        in_specs=[smem] + [vmem] * 3,
        out_specs=(vmem, vmem),
        compiler_params=pltpu.CompilerParams(vmem_limit_bytes=24 << 20),
        name="grads",
    )(core, pre, feats, second)


def finish_kernel(pieces_ref, first_ref, second_ref):
    total = jnp.sum(pieces_ref[...].astype(F32), axis=0)
    lead = second_ref.shape[1]
    second_ref[...] = total[:, :lead]
    first_ref[...] = total[:, lead:]


def make_finish(pieces, lead):
    vmem = pl.BlockSpec(memory_space=pltpu.VMEM)
    rows, width = pieces.shape[1:]
    return pl.pallas_call(
        finish_kernel,
        out_shape=(
            jax.ShapeDtypeStruct((rows, width - lead), F32),
            jax.ShapeDtypeStruct((rows, lead), F32),
        ),
        in_specs=[vmem],
        out_specs=(vmem, vmem),
        compiler_params=pltpu.CompilerParams(vmem_limit_bytes=8 << 20),
        name="finish",
    )(pieces)


def swapped(parts, axis):
    return lax.all_to_all(parts, axis, split_axis=0, concat_axis=0, tiled=True)


def per_device(sizes, proposal_boxes, level_plan, fine_map, coarse_map, first_weight,
               second_weight, upstream):
    nx, nz, nc, tile_count = sizes
    dp = ("x", "z", "core")
    dp_count = nx * nz * nc
    band = lax.axis_index("tile")
    fine = fine_map[0]
    coarse = coarse_map[0]
    up = [(i + 1, i) for i in range(tile_count - 1)]
    fine_top, coarse_top = cut_tops(fine, coarse)
    fine_below = lax.ppermute(fine_top, "tile", up)
    coarse_below = lax.ppermute(coarse_top, "tile", up)
    mine = lax.axis_index("core")
    band_at = band[None].astype(jnp.int32)
    num_props = level_plan.shape[1]
    capacity = max(num_props // 4, num_props // tile_count)
    unit = first_weight.shape[1]
    lead = second_weight.shape[0]
    upstream_rows = upstream[0]

    slot_id, ints, reals = make_plan(
        band_at, proposal_boxes[0], level_plan, tile_count, capacity, fine.shape[0],
        coarse.shape[0], 4,
    )
    early, edge = make_crops(ints, reals, fine, coarse, band_at, tile_count)
    copies = make_copies(first_weight.T, second_weight.T, dp_count)
    weights = swapped(copies, dp).reshape(-1, copies.shape[2])
    crops = edge(early, fine_below, coarse_below)
    recvs = {0: crops[0]}
    for k in range(1, tile_count):
        route = [(i, (i + k) % tile_count) for i in range(tile_count)]
        recvs[k] = lax.ppermute(crops[k], "tile", route)
    gather_at = jnp.stack([band, jnp.int32(tile_count)]).astype(jnp.int32)
    soon, late = (0, *TURNS[:4]), TURNS[4:]
    begun = make_gather(gather_at, slot_id, [recvs[k] for k in soon], soon)
    weights, begun = lax.optimization_barrier((weights, begun))
    back_grad = lax.dot_general(
        weights[:, :lead], upstream_rows, (((0,), (1,)), ((), ())), preferred_element_type=F32
    )
    back_grad, weights = lax.optimization_barrier((back_grad, weights))
    feats, partial_hidden = make_hidden(
        gather_at, slot_id, weights, begun, [recvs[k] for k in late], late
    )
    pieces = swapped(partial_hidden.reshape(tile_count, -1, num_props), "tile")
    activated, copies = make_act(pieces, back_grad)
    pre_grad = swapped(copies, "tile").reshape(-1, num_props)
    second = lax.dot_general(
        upstream_rows, activated, (((0,), (1,)), ((), ())), preferred_element_type=F32
    ).astype(BF)
    core_at = mine[None].astype(jnp.int32)
    keep, give = make_grads(core_at, pre_grad, feats, second, unit)
    got = lax.ppermute(give, "core", [(0, 1), (1, 0)])
    both = (keep.astype(F32) + got.astype(F32)).astype(BF).reshape(nx, nz, unit, -1)
    total = swapped(both, "x").astype(F32).sum(axis=0)
    first_grad, second_grad = make_finish(swapped(total.astype(BF), "z"), lead)
    return (first_grad.T, second_grad.T)


def solution(mesh):
    tile_count = mesh.shape["tile"]
    sizes = (4, mesh.shape["dp"] // 8, 2, tile_count)
    split = Mesh(mesh.devices.reshape(sizes), ("x", "z", "core", "tile"))
    dp = ("x", "z", "core")
    placed = (
        P(dp, None, None),
        P(dp, None),
        P(dp, "tile", None, None),
        P(dp, "tile", None, None),
        P("tile", dp),
        P("tile", dp),
        P(dp, None, None),
    )

    def step(*args):
        return per_device(sizes, *args)

    return jax.shard_map(
        step,
        mesh=split,
        in_specs=placed,
        out_specs=(P("tile", dp), P("tile", dp)),
        check_vma=False,
    )
```

```python
import jax
import jax.numpy as jnp
from jax import lax
from jax.experimental import pallas as pl
from jax.experimental.pallas import tpu as pltpu
from jax.sharding import Mesh, PartitionSpec as P


REACH = 14
SPAN = 32
GROUP = 8
TURNS = (4, 7, 1, 6, 2, 5, 3)
BF = jnp.bfloat16
F32 = jnp.float32


def gelu_parts(hidden):
    factor = 0.7978845608028654
    cubic_term = 0.044715
    inner_term = factor * (hidden + cubic_term * hidden * hidden * hidden)
    tangent = jnp.tanh(inner_term)
    gelu_value = 0.5 * hidden * (1.0 + tangent)
    gelu_slope = 0.5 * (1.0 + tangent) + 0.5 * hidden * (1.0 - tangent * tangent) * factor * (
        1.0 + 3.0 * cubic_term * hidden * hidden
    )
    return (gelu_value, gelu_slope)


def top_kernel(fine_ref, coarse_ref, fine_top_ref, coarse_top_ref, arrived):
    moves = [
        pltpu.make_async_copy(fine_ref.at[0:REACH], fine_top_ref, arrived.at[0]),
        pltpu.make_async_copy(coarse_ref.at[0:REACH], coarse_top_ref, arrived.at[1]),
    ]
    for move in moves:
        move.start()
    for move in moves:
        move.wait()


def cut_tops(fine, coarse):
    away = pl.BlockSpec(memory_space=pltpu.HBM)
    return pl.pallas_call(
        top_kernel,
        out_shape=(
            jax.ShapeDtypeStruct((REACH, *fine.shape[1:]), BF),
            jax.ShapeDtypeStruct((REACH, *coarse.shape[1:]), BF),
        ),
        in_specs=[away, away],
        out_specs=(pl.BlockSpec(memory_space=pltpu.VMEM), pl.BlockSpec(memory_space=pltpu.VMEM)),
        scratch_shapes=[pltpu.SemaphoreType.DMA((2,))],
        compiler_params=pltpu.CompilerParams(vmem_limit_bytes=60 << 20),
        name="tops",
    )(fine, coarse)


def copies_kernel(first_ref, second_ref, out_ref):
    lead = second_ref.shape[1]
    first = first_ref[...]
    second = second_ref[...]

    def body(i, carry):
        out_ref[i, :, 0:lead] = second
        out_ref[i, :, lead:] = first
        return carry

    lax.fori_loop(0, out_ref.shape[0], body, 0)


def make_copies(first, second, count):
    vmem = pl.BlockSpec(memory_space=pltpu.VMEM)
    width = first.shape[1] + second.shape[1]
    return pl.pallas_call(
        copies_kernel,
        out_shape=jax.ShapeDtypeStruct((count, first.shape[0], width), BF),
        in_specs=[vmem, vmem],
        out_specs=vmem,
        compiler_params=pltpu.CompilerParams(vmem_limit_bytes=8 << 20),
        name="copies",
    )(first, second)


def plan_kernel(band_ref, box_ref, level_ref, slot_ref, ints_ref, reals_ref, *, shape):
    tiles, capacity, fine_rows, coarse_rows, stride = shape
    props = level_ref.shape[1]
    band = band_ref[0]
    top, left, height, width = (box_ref[i : i + 1, :] for i in range(4))
    level = level_ref[...]
    rows_px = stride * fine_rows
    owner = jnp.zeros_like(top)
    for b in range(1, tiles):
        owner = owner + jnp.where(top >= b * rows_px, 1, 0)
    down = (top - owner * rows_px).astype(F32)
    scale = jnp.where(level == 0, 1.0 / stride, 0.5 / stride)
    last = down * scale + 6.5 * height.astype(F32) * (scale / 7.0)
    limit = jnp.where(level == 0, float(fine_rows), float(coarse_rows))
    crosses = jnp.where(last >= limit - 1.01, 1.0, 0.0)
    inside = lax.broadcasted_iota(jnp.int32, (tiles, props), 0) == owner
    late = jnp.where(inside, crosses, 0.0)
    early = jnp.where(inside, 1.0 - crosses, 0.0)
    upto = lax.broadcasted_iota(jnp.int32, (props, props), 0) <= lax.broadcasted_iota(
        jnp.int32, (props, props), 1
    )
    upto = jnp.where(upto, 1.0, 0.0).astype(BF)
    both = jnp.concatenate([early, late], axis=0).astype(BF)
    order = jnp.dot(both, upto, preferred_element_type=F32)
    first = jnp.sum(early, axis=1, keepdims=True)
    every = first + jnp.sum(late, axis=1, keepdims=True)
    rank = early * (order[:tiles] - 1.0) + late * (order[tiles:] + first - 1.0)
    rank = jnp.sum(rank, axis=0, keepdims=True).astype(jnp.int32)
    slot = owner * capacity + rank
    slot_ref[...] = slot
    here = lax.broadcasted_iota(jnp.int32, (capacity, props), 0) + band * capacity == slot
    here = jnp.where(here, 1.0, 0.0).astype(BF)
    fields = jnp.concatenate(
        [
            down,
            (left // 8).astype(F32),
            (left % 8).astype(F32),
            height.astype(F32),
            width.astype(F32),
            level.astype(F32),
            jnp.ones_like(down),
            jnp.zeros_like(down),
        ],
        axis=0,
    ).astype(BF)
    fields = jnp.concatenate([fields, jnp.zeros_like(fields)], axis=0)
    taken = lax.dot_general(fields, here, (((1,), (1,)), ((), ())), preferred_element_type=F32)
    down, left_high, left_low, height, width, level, live = (taken[i : i + 1] for i in range(7))
    scale = jnp.where(level > 0.5, 0.5 / stride, 1.0 / stride)
    step = lax.broadcasted_iota(jnp.int32, (8, capacity), 0).astype(F32) + 0.5
    point = down * scale + step * (height * (scale / 7.0))
    whole = jnp.floor(point)
    near = jnp.maximum(0.0, 1.0 - (point - whole)).astype(BF).astype(F32)
    far = jnp.maximum(0.0, 1.0 - (whole + 1.0 - point)).astype(BF).astype(F32)
    most = jnp.where(level > 0.5, float(coarse_rows), float(fine_rows)) + (REACH - 2.0)
    whole = jnp.clip(whole, 0.0, most) + jnp.where(level > 0.5, fine_rows + float(REACH), 0.0)
    across = (left_high * 8.0 + left_low) * scale
    col = jnp.floor(across * 0.0625) * 16.0
    own = lax.broadcasted_iota(jnp.int32, (tiles, 1), 0) == band
    early_count = jnp.sum(jnp.where(own, first, 0.0), axis=0, keepdims=True)
    every_count = jnp.sum(jnp.where(own, every, 0.0), axis=0, keepdims=True)
    at = lax.broadcasted_iota(jnp.int32, (8, capacity), 0)
    extra = jnp.where(at == 0, col, jnp.where(at == 1, early_count, every_count))
    ints_ref[0:8] = whole.astype(jnp.int32)
    ints_ref[8:16] = extra.astype(jnp.int32)
    reals_ref[0:8] = near * live
    reals_ref[8:16] = far * live
    reals_ref[16:24] = jnp.where(at == 0, across - col, width * (scale / 7.0))


def make_plan(band, boxes, levels, tiles, capacity, fine_rows, coarse_rows, stride):
    smem = pl.BlockSpec(memory_space=pltpu.SMEM)
    vmem = pl.BlockSpec(memory_space=pltpu.VMEM)

    def kernel(*refs):
        plan_kernel(*refs, shape=(tiles, capacity, fine_rows, coarse_rows, stride))

    return pl.pallas_call(
        kernel,
        out_shape=(
            jax.ShapeDtypeStruct(levels.shape, jnp.int32),
            jax.ShapeDtypeStruct((16, capacity), jnp.int32),
            jax.ShapeDtypeStruct((24, capacity), F32),
        ),
        in_specs=[smem, vmem, vmem],
        out_specs=(vmem, vmem, vmem),
        compiler_params=pltpu.CompilerParams(vmem_limit_bytes=8 << 20),
        name="plan",
    )(band, boxes, levels)


def fill_maps(maps, fine_ref, coarse_ref, below, arrived):
    fine_rows, fine_cols, channels = fine_ref.shape
    coarse_rows, coarse_cols, _ = coarse_ref.shape
    total, pitch, _ = maps.shape
    base = fine_rows + REACH
    fine_copy = pltpu.make_async_copy(
        fine_ref, maps.at[0:fine_rows, 0:fine_cols, :], arrived.at[0]
    )
    fine_copy.start()
    maps[0:base, fine_cols:pitch, :] = jnp.zeros((base, pitch - fine_cols, channels), BF)
    maps[base:total, :, :] = jnp.zeros((total - base, pitch, channels), BF)
    maps[base : base + coarse_rows, 0:coarse_cols, :] = coarse_ref[...]
    if below is None:
        maps[fine_rows:base, 0:fine_cols, :] = jnp.zeros((REACH, fine_cols, channels), BF)
    else:
        maps[fine_rows:base, 0:fine_cols, :] = below[0][...]
        maps[base + coarse_rows : total, 0:coarse_cols, :] = below[1][...]
    fine_copy.wait()


def fill_cells(bin_ref, cell_ref):
    line = lax.broadcasted_iota(jnp.int32, bin_ref.shape, 0)
    lane = lax.broadcasted_iota(jnp.int32, bin_ref.shape, 1)
    bin_ref[...] = line.astype(F32) + 0.5
    cell_ref[...] = (lane % SPAN).astype(F32)


def crop_group(step, ints_ref, reals_ref, bin_ref, cell_ref, maps, parts, crops):
    channels = maps.shape[2]
    bins = parts.shape[1]
    first = step * GROUP
    for g in range(GROUP):
        slot = first + g
        col = pl.multiple_of(ints_ref[8, slot], 16)
        lines = []
        for i in range(7):
            row = ints_ref[i, slot]
            upper = maps[row, pl.ds(col, SPAN), :]
            lower = maps[row + 1, pl.ds(col, SPAN), :]
            near = jnp.full(upper.shape, reals_ref[i, slot], F32).astype(BF)
            far = jnp.full(upper.shape, reals_ref[8 + i, slot], F32).astype(BF)
            lines.append(near * upper + far * lower)
        lines.append(jnp.zeros((SPAN, channels), BF))
        stacked = jnp.concatenate(lines, axis=0)
        away = (reals_ref[16, slot] + bin_ref[...] * reals_ref[17, slot]) - cell_ref[...]
        line = jnp.maximum(0.0, 1.0 - jnp.abs(away))
        piece = lax.broadcasted_iota(jnp.int32, line.shape, 1) // SPAN
        mix = [jnp.where(piece == i, line, 0.0) for i in range(7)]
        mix = jnp.concatenate(mix, axis=0).astype(BF)
        parts[g] = jnp.dot(mix, stacked, preferred_element_type=F32)
    flat = parts.reshape(GROUP * bins, channels)
    start = pl.multiple_of(first, GROUP)
    for m in range(49):
        at = m // 7 * 8 + m % 7
        crops[m, pl.ds(start, GROUP), :] = flat[pl.ds(at, GROUP, stride=bins), :]


def inner_kernel(ints_ref, reals_ref, fine_ref, coarse_ref, crops_ref, maps, parts, bin_ref,
                 cell_ref, arrived):
    fill_cells(bin_ref, cell_ref)
    fill_maps(maps, fine_ref, coarse_ref, None, arrived)

    def body(step, carry):
        crop_group(step, ints_ref, reals_ref, bin_ref, cell_ref, maps, parts, crops_ref)
        return carry

    lax.fori_loop(0, crops_ref.shape[1] // GROUP, body, 0)


def edge_kernel(ints_ref, reals_ref, fine_ref, coarse_ref, fine_below_ref, coarse_below_ref,
                inner_ref, band_ref, *rest):
    *outs, maps, parts, bin_ref, cell_ref, arrived, crops, early, flipped = rest
    channels = fine_ref.shape[2]
    early_copy = pltpu.make_async_copy(inner_ref, early, arrived.at[1])
    early_copy.start()
    fill_cells(bin_ref, cell_ref)
    fill_maps(maps, fine_ref, coarse_ref, (fine_below_ref, coarse_below_ref), arrived)
    low = ints_ref[9, 0] // GROUP
    high = (ints_ref[10, 0] + (GROUP - 1)) // GROUP

    def body(step, carry):
        crop_group(step, ints_ref, reals_ref, bin_ref, cell_ref, maps, parts, crops)
        return carry

    lax.fori_loop(low, high, body, 0)
    early_copy.wait()
    at = lax.broadcasted_iota(jnp.int32, (crops.shape[1], channels), 0)
    redone = (at >= low * GROUP) & (at < high * GROUP)
    for m in range(49):
        block = jnp.where(redone, crops[m], early[m])
        flipped[m * channels : (m + 1) * channels, :] = block.T.astype(BF)
    share = outs[0].shape[0]
    for k, out in enumerate(outs):
        block = (band_ref[0] + k) % len(outs)
        out[...] = flipped[pl.ds(pl.multiple_of(block * share, 16), share), :]


def make_crops(ints, reals, fine, coarse, band, tiles):
    capacity = ints.shape[1]
    channels = fine.shape[2]
    total = fine.shape[0] + coarse.shape[0] + 2 * REACH
    smem = pl.BlockSpec(memory_space=pltpu.SMEM)
    vmem = pl.BlockSpec(memory_space=pltpu.VMEM)
    away = pl.BlockSpec(memory_space=pltpu.HBM)
    common = [
        pltpu.VMEM((total, 192, channels), BF),
        pltpu.VMEM((GROUP, 56, channels), F32),
        pltpu.VMEM((8, 8 * SPAN), F32),
        pltpu.VMEM((8, 8 * SPAN), F32),
        pltpu.SemaphoreType.DMA((2,)),
    ]
    every = jax.ShapeDtypeStruct((49, capacity, channels), F32)
    params = pltpu.CompilerParams(vmem_limit_bytes=24 << 20)
    inner = pl.pallas_call(
        inner_kernel,
        out_shape=every,
        in_specs=[smem, smem, away, vmem],
        out_specs=vmem,
        scratch_shapes=common,
        compiler_params=params,
        name="inner",
    )
    edge = pl.pallas_call(
        edge_kernel,
        out_shape=[jax.ShapeDtypeStruct((49 * channels // tiles, capacity), BF)] * tiles,
        in_specs=[smem, smem, away, vmem, vmem, vmem, away, smem],
        out_specs=[vmem] * tiles,
        scratch_shapes=common
        + [
            pltpu.VMEM(every.shape, F32),
            pltpu.VMEM(every.shape, F32),
            pltpu.VMEM((49 * channels, capacity), BF),
        ],
        compiler_params=params,
        name="edge",
    )
    early = inner(ints, reals, fine, coarse)
    return early, lambda early, fine_below, coarse_below: edge(
        ints, reals, fine, coarse, fine_below, coarse_below, early, band
    )


def pick_rows(turns, band_ref, slot_ref, recvs, joined, pick, arrived):
    count, capacity = band_ref[1], recvs[0].shape[1]
    slots = slot_ref[...]
    moves = [
        pltpu.make_async_copy(
            recv, joined.at[:, k * capacity : (k + 1) * capacity], arrived.at[k]
        )
        for k, recv in enumerate(recvs)
    ]
    for move in moves:
        move.start()
    for k, turn in enumerate(turns):
        source = (band_ref[0] + count - turn) % count
        at = lax.broadcasted_iota(jnp.int32, (capacity, slots.shape[1]), 0) + source * capacity
        pick[k * capacity : (k + 1) * capacity, :] = jnp.where(at == slots, 1.0, 0.0).astype(BF)
    for move in moves:
        move.wait()
    return jnp.dot(joined[...], pick[...], preferred_element_type=F32)


def make_gather(band, slot_id, recvs, turns):
    share, capacity = recvs[0].shape
    props = slot_id.shape[1]
    count = len(recvs)
    smem = pl.BlockSpec(memory_space=pltpu.SMEM)
    vmem = pl.BlockSpec(memory_space=pltpu.VMEM)

    def gather_kernel(band_ref, slot_ref, *rest):
        *pieces, out_ref, joined, pick, arrived = rest
        out_ref[...] = pick_rows(turns, band_ref, slot_ref, pieces, joined, pick, arrived).astype(BF)

    return pl.pallas_call(
        gather_kernel,
        out_shape=jax.ShapeDtypeStruct((share, props), BF),
        in_specs=[smem, vmem] + [pl.BlockSpec(memory_space=pl.ANY)] * count,
        out_specs=vmem,
        scratch_shapes=[
            pltpu.VMEM((share, count * capacity), BF),
            pltpu.VMEM((count * capacity, props), BF),
            pltpu.SemaphoreType.DMA((count,)),
        ],
        compiler_params=pltpu.CompilerParams(vmem_limit_bytes=16 << 20),
        name="gather",
    )(band, slot_id, *recvs)


def make_hidden(band, slot_id, weight, begun, recvs, turns):
    share, capacity = recvs[0].shape
    props = slot_id.shape[1]
    count = len(recvs)
    smem = pl.BlockSpec(memory_space=pltpu.SMEM)
    vmem = pl.BlockSpec(memory_space=pltpu.VMEM)

    def hidden_kernel(band_ref, slot_ref, weight_ref, begun_ref, *rest):
        *pieces, feats_ref, out_ref, joined, pick, arrived = rest
        late = pick_rows(turns, band_ref, slot_ref, pieces, joined, pick, arrived)
        feats_ref[...] = begun_ref[...] + late.astype(BF)
        skip = weight_ref.shape[1] - share
        out_ref[...] = jnp.dot(
            weight_ref[:, skip:], feats_ref[...], preferred_element_type=F32
        ).astype(BF)

    return pl.pallas_call(
        hidden_kernel,
        out_shape=(
            jax.ShapeDtypeStruct((share, props), BF),
            jax.ShapeDtypeStruct((weight.shape[0], props), BF),
        ),
        in_specs=[smem, vmem, vmem, vmem] + [pl.BlockSpec(memory_space=pl.ANY)] * count,
        out_specs=(vmem, vmem),
        scratch_shapes=[
            pltpu.VMEM((share, count * capacity), BF),
            pltpu.VMEM((count * capacity, props), BF),
            pltpu.SemaphoreType.DMA((count,)),
        ],
        compiler_params=pltpu.CompilerParams(vmem_limit_bytes=24 << 20),
        name="hidden",
    )(band, slot_id, weight, begun, *recvs)


def act_kernel(pieces_ref, back_ref, act_ref, pre_ref):
    hidden = jnp.sum(pieces_ref[...].astype(F32), axis=0)
    value, slope = gelu_parts(hidden)
    act_ref[...] = value.astype(BF)
    pre = (back_ref[...] * slope).astype(BF)
    for t in range(pre_ref.shape[0]):
        pre_ref[t] = pre


def make_act(pieces, back):
    vmem = pl.BlockSpec(memory_space=pltpu.VMEM)
    return pl.pallas_call(
        act_kernel,
        out_shape=(
            jax.ShapeDtypeStruct(pieces.shape[1:], BF),
            jax.ShapeDtypeStruct(pieces.shape, BF),
        ),
        in_specs=[vmem, vmem],
        out_specs=(vmem, vmem),
        compiler_params=pltpu.CompilerParams(vmem_limit_bytes=8 << 20),
        name="act",
    )(pieces, back)


def grads_kernel(core_ref, pre_ref, feats_ref, keep_ref, give_ref):
    rows = 256
    unit = keep_ref.shape[1]
    mine = core_ref[0] == 0

    def block(step, carry):
        start = pl.multiple_of(step * rows, rows)
        first = lax.dot_general(
            pre_ref[pl.ds(start, rows), :], feats_ref[...], (((1,), (1,)), ((), ())),
            preferred_element_type=F32,
        ).astype(BF)
        for n in range(rows // (2 * unit)):
            at = step * (rows // (2 * unit)) + n
            even = first[2 * n * unit : (2 * n + 1) * unit]
            odd = first[(2 * n + 1) * unit : (2 * n + 2) * unit]
            keep_ref[at] = jnp.where(mine, even, odd)
            give_ref[at] = jnp.where(mine, odd, even)
        return carry

    lax.fori_loop(0, pre_ref.shape[0] // rows, block, 0)


def make_grads(core, pre, feats, unit):
    smem = pl.BlockSpec(memory_space=pltpu.SMEM)
    vmem = pl.BlockSpec(memory_space=pltpu.VMEM)
    half = jax.ShapeDtypeStruct((pre.shape[0] // (2 * unit), unit, feats.shape[0]), BF)
    return pl.pallas_call(
        grads_kernel,
        out_shape=(half, half),
        in_specs=[smem, vmem, vmem],
        out_specs=(vmem, vmem),
        compiler_params=pltpu.CompilerParams(vmem_limit_bytes=24 << 20),
        name="grads",
    )(core, pre, feats)


def total_kernel(*refs):
    *parts, out_ref = refs
    out_ref[...] = sum(part[...].astype(F32) for part in parts).astype(BF)


def make_total(parts):
    vmem = pl.BlockSpec(memory_space=pltpu.VMEM)
    return pl.pallas_call(
        total_kernel,
        out_shape=jax.ShapeDtypeStruct(parts[0].shape, BF),
        in_specs=[vmem] * len(parts),
        out_specs=vmem,
        compiler_params=pltpu.CompilerParams(vmem_limit_bytes=4 << 20),
        name="total",
    )(*parts)


def merge_kernel(pieces_ref, second_ref, out_ref):
    lead = second_ref.shape[2]
    out_ref[:, :, 0:lead] = second_ref[...]
    out_ref[:, :, lead:] = jnp.sum(pieces_ref[...].astype(F32), axis=0).astype(BF)


def make_merge(pieces, second):
    vmem = pl.BlockSpec(memory_space=pltpu.VMEM)
    groups, unit, width = pieces.shape[1:]
    return pl.pallas_call(
        merge_kernel,
        out_shape=jax.ShapeDtypeStruct((groups, unit, width + second.shape[2]), BF),
        in_specs=[vmem, vmem],
        out_specs=vmem,
        compiler_params=pltpu.CompilerParams(vmem_limit_bytes=8 << 20),
        name="merge",
    )(pieces, second)


def finish_kernel(pieces_ref, first_ref, second_ref):
    total = jnp.sum(pieces_ref[...].astype(F32), axis=0)
    lead = second_ref.shape[1]
    second_ref[...] = total[:, :lead]
    first_ref[...] = total[:, lead:]


def make_finish(pieces, lead):
    vmem = pl.BlockSpec(memory_space=pltpu.VMEM)
    rows, width = pieces.shape[1:]
    return pl.pallas_call(
        finish_kernel,
        out_shape=(
            jax.ShapeDtypeStruct((rows, width - lead), F32),
            jax.ShapeDtypeStruct((rows, lead), F32),
        ),
        in_specs=[vmem],
        out_specs=(vmem, vmem),
        compiler_params=pltpu.CompilerParams(vmem_limit_bytes=8 << 20),
        name="finish",
    )(pieces)


def swapped(parts, axis):
    return lax.all_to_all(parts, axis, split_axis=0, concat_axis=0, tiled=True)


def per_device(sizes, proposal_boxes, level_plan, fine_map, coarse_map, first_weight,
               second_weight, upstream):
    nx, nz, nc, tile_count = sizes
    dp = ("x", "z", "core")
    dp_count = nx * nz * nc
    band = lax.axis_index("tile")
    fine = fine_map[0]
    coarse = coarse_map[0]
    up = [(i + 1, i) for i in range(tile_count - 1)]
    fine_top, coarse_top = cut_tops(fine, coarse)
    fine_below = lax.ppermute(fine_top, "tile", up)
    coarse_below = lax.ppermute(coarse_top, "tile", up)
    mine = lax.axis_index("core")
    band_at = band[None].astype(jnp.int32)
    num_props = level_plan.shape[1]
    capacity = max(num_props // 4, num_props // tile_count)
    unit = first_weight.shape[1]
    lead = second_weight.shape[0]
    upstream_rows = upstream[0]

    slot_id, ints, reals = make_plan(
        band_at, proposal_boxes[0], level_plan, tile_count, capacity, fine.shape[0],
        coarse.shape[0], 4,
    )
    early, edge = make_crops(ints, reals, fine, coarse, band_at, tile_count)
    copies = make_copies(first_weight.T, second_weight.T, dp_count)
    weights = swapped(copies, dp).reshape(-1, copies.shape[2])
    crops = edge(early, fine_below, coarse_below)
    recvs = {0: crops[0]}
    for k in range(1, tile_count):
        route = [(i, (i + k) % tile_count) for i in range(tile_count)]
        recvs[k] = lax.ppermute(crops[k], "tile", route)
    gather_at = jnp.stack([band, jnp.int32(tile_count)]).astype(jnp.int32)
    soon, late = (0, *TURNS[:4]), TURNS[4:]
    begun = make_gather(gather_at, slot_id, [recvs[k] for k in soon], soon)
    weights, begun = lax.optimization_barrier((weights, begun))
    back_grad = lax.dot_general(
        weights[:, :lead], upstream_rows, (((0,), (1,)), ((), ())), preferred_element_type=F32
    )
    back_grad, weights = lax.optimization_barrier((back_grad, weights))
    feats, partial_hidden = make_hidden(
        gather_at, slot_id, weights, begun, [recvs[k] for k in late], late
    )
    pieces = swapped(partial_hidden.reshape(tile_count, -1, num_props), "tile")
    activated, copies = make_act(pieces, back_grad)
    pre_grad = swapped(copies, "tile").reshape(-1, num_props)
    second = lax.dot_general(
        upstream_rows, activated, (((0,), (1,)), ((), ())), preferred_element_type=F32
    )
    second = second.astype(BF).reshape(nx, nz, nc, unit, -1)
    second_keep = jnp.where(mine == 0, second[:, :, 0], second[:, :, 1])
    second_give = jnp.where(mine == 0, second[:, :, 1], second[:, :, 0])
    second_got = lax.ppermute(second_give, "core", [(0, 1), (1, 0)])
    second_both = (second_keep.astype(F32) + second_got.astype(F32)).astype(BF)
    place = lax.axis_index("x")
    parts = []
    for k in range(nx):
        part = lax.dynamic_index_in_dim(second_both, (place + k) % nx, 0, keepdims=False)
        if k > 0:
            part = lax.ppermute(part, "x", [(i, (i + k) % nx) for i in range(nx)])
        parts.append(part)
    second_total = make_total(parts)
    core_at = mine[None].astype(jnp.int32)
    keep, give = make_grads(core_at, pre_grad, feats, unit)
    got = lax.ppermute(give, "core", [(0, 1), (1, 0)])
    both = (keep.astype(F32) + got.astype(F32)).astype(BF).reshape(nx, nz, unit, -1)
    total = make_merge(swapped(both, "x"), second_total)
    first_grad, second_grad = make_finish(swapped(total, "z"), lead)
    return (first_grad.T, second_grad.T)


def solution(mesh):
    tile_count = mesh.shape["tile"]
    sizes = (4, mesh.shape["dp"] // 8, 2, tile_count)
    split = Mesh(mesh.devices.reshape(sizes), ("x", "z", "core", "tile"))
    dp = ("x", "z", "core")
    placed = (
        P(dp, None, None),
        P(dp, None),
        P(dp, "tile", None, None),
        P(dp, "tile", None, None),
        P("tile", dp),
        P("tile", dp),
        P(dp, None, None),
    )

    def step(*args):
        return per_device(sizes, *args)

    return jax.shard_map(
        step,
        mesh=split,
        in_specs=placed,
        out_specs=(P("tile", dp), P("tile", dp)),
        check_vma=False,
    )
```

```python
import jax
import jax.numpy as jnp
from jax import lax
from jax.experimental import pallas as pl
from jax.experimental.pallas import tpu as pltpu
from jax.sharding import Mesh, PartitionSpec as P


REACH = 14
SPAN = 32
GROUP = 8
TURNS = (4, 7, 1, 6, 2, 5, 3)
BF = jnp.bfloat16
F32 = jnp.float32


def gelu_parts(hidden):
    factor = 0.7978845608028654
    cubic_term = 0.044715
    inner_term = factor * (hidden + cubic_term * hidden * hidden * hidden)
    tangent = jnp.tanh(inner_term)
    gelu_value = 0.5 * hidden * (1.0 + tangent)
    gelu_slope = 0.5 * (1.0 + tangent) + 0.5 * hidden * (1.0 - tangent * tangent) * factor * (
        1.0 + 3.0 * cubic_term * hidden * hidden
    )
    return (gelu_value, gelu_slope)


def top_kernel(fine_ref, coarse_ref, fine_top_ref, coarse_top_ref, arrived):
    moves = [
        pltpu.make_async_copy(fine_ref.at[0:REACH], fine_top_ref, arrived.at[0]),
        pltpu.make_async_copy(coarse_ref.at[0:REACH], coarse_top_ref, arrived.at[1]),
    ]
    for move in moves:
        move.start()
    for move in moves:
        move.wait()


def cut_tops(fine, coarse):
    away = pl.BlockSpec(memory_space=pltpu.HBM)
    return pl.pallas_call(
        top_kernel,
        out_shape=(
            jax.ShapeDtypeStruct((REACH, *fine.shape[1:]), BF),
            jax.ShapeDtypeStruct((REACH, *coarse.shape[1:]), BF),
        ),
        in_specs=[away, away],
        out_specs=(pl.BlockSpec(memory_space=pltpu.VMEM), pl.BlockSpec(memory_space=pltpu.VMEM)),
        scratch_shapes=[pltpu.SemaphoreType.DMA((2,))],
        compiler_params=pltpu.CompilerParams(vmem_limit_bytes=60 << 20),
        name="tops",
    )(fine, coarse)


def copies_kernel(first_ref, second_ref, out_ref, joined, sent):
    lead = second_ref.shape[1]
    joined[:, 0:lead] = second_ref[...]
    joined[:, lead:] = first_ref[...]
    moves = [
        pltpu.make_async_copy(joined, out_ref.at[i], sent.at[i]) for i in range(out_ref.shape[0])
    ]
    for move in moves:
        move.start()
    for move in moves:
        move.wait()


def make_copies(first, second, count):
    vmem = pl.BlockSpec(memory_space=pltpu.VMEM)
    width = first.shape[1] + second.shape[1]
    return pl.pallas_call(
        copies_kernel,
        out_shape=jax.ShapeDtypeStruct((count, first.shape[0], width), BF),
        in_specs=[vmem, vmem],
        out_specs=pl.BlockSpec(memory_space=pltpu.HBM),
        scratch_shapes=[
            pltpu.VMEM((first.shape[0], width), BF),
            pltpu.SemaphoreType.DMA((count,)),
        ],
        compiler_params=pltpu.CompilerParams(vmem_limit_bytes=8 << 20),
        name="copies",
    )(first, second)


def plan_kernel(band_ref, box_ref, level_ref, slot_ref, ints_ref, reals_ref, *, shape):
    tiles, capacity, fine_rows, coarse_rows, stride = shape
    props = level_ref.shape[1]
    band = band_ref[0]
    top, left, height, width = (box_ref[i : i + 1, :] for i in range(4))
    level = level_ref[...]
    rows_px = stride * fine_rows
    owner = jnp.zeros_like(top)
    for b in range(1, tiles):
        owner = owner + jnp.where(top >= b * rows_px, 1, 0)
    down = (top - owner * rows_px).astype(F32)
    scale = jnp.where(level == 0, 1.0 / stride, 0.5 / stride)
    last = down * scale + 6.5 * height.astype(F32) * (scale / 7.0)
    limit = jnp.where(level == 0, float(fine_rows), float(coarse_rows))
    crosses = jnp.where(last >= limit - 1.01, 1.0, 0.0)
    inside = lax.broadcasted_iota(jnp.int32, (tiles, props), 0) == owner
    late = jnp.where(inside, crosses, 0.0)
    early = jnp.where(inside, 1.0 - crosses, 0.0)
    upto = lax.broadcasted_iota(jnp.int32, (props, props), 0) <= lax.broadcasted_iota(
        jnp.int32, (props, props), 1
    )
    upto = jnp.where(upto, 1.0, 0.0).astype(BF)
    both = jnp.concatenate([early, late], axis=0).astype(BF)
    order = jnp.dot(both, upto, preferred_element_type=F32)
    first = jnp.sum(early, axis=1, keepdims=True)
    every = first + jnp.sum(late, axis=1, keepdims=True)
    rank = early * (order[:tiles] - 1.0) + late * (order[tiles:] + first - 1.0)
    rank = jnp.sum(rank, axis=0, keepdims=True).astype(jnp.int32)
    slot = owner * capacity + rank
    slot_ref[...] = slot
    here = lax.broadcasted_iota(jnp.int32, (capacity, props), 0) + band * capacity == slot
    here = jnp.where(here, 1.0, 0.0).astype(BF)
    fields = jnp.concatenate(
        [
            down,
            (left // 8).astype(F32),
            (left % 8).astype(F32),
            height.astype(F32),
            width.astype(F32),
            level.astype(F32),
            jnp.ones_like(down),
            jnp.zeros_like(down),
        ],
        axis=0,
    ).astype(BF)
    fields = jnp.concatenate([fields, jnp.zeros_like(fields)], axis=0)
    taken = lax.dot_general(fields, here, (((1,), (1,)), ((), ())), preferred_element_type=F32)
    down, left_high, left_low, height, width, level, live = (taken[i : i + 1] for i in range(7))
    scale = jnp.where(level > 0.5, 0.5 / stride, 1.0 / stride)
    step = lax.broadcasted_iota(jnp.int32, (8, capacity), 0).astype(F32) + 0.5
    point = down * scale + step * (height * (scale / 7.0))
    whole = jnp.floor(point)
    near = jnp.maximum(0.0, 1.0 - (point - whole)).astype(BF).astype(F32)
    far = jnp.maximum(0.0, 1.0 - (whole + 1.0 - point)).astype(BF).astype(F32)
    most = jnp.where(level > 0.5, float(coarse_rows), float(fine_rows)) + (REACH - 2.0)
    whole = jnp.clip(whole, 0.0, most) + jnp.where(level > 0.5, fine_rows + float(REACH), 0.0)
    across = (left_high * 8.0 + left_low) * scale
    col = jnp.floor(across * 0.0625) * 16.0
    own = lax.broadcasted_iota(jnp.int32, (tiles, 1), 0) == band
    early_count = jnp.sum(jnp.where(own, first, 0.0), axis=0, keepdims=True)
    every_count = jnp.sum(jnp.where(own, every, 0.0), axis=0, keepdims=True)
    at = lax.broadcasted_iota(jnp.int32, (8, capacity), 0)
    extra = jnp.where(at == 0, col, jnp.where(at == 1, early_count, every_count))
    ints_ref[0:8] = whole.astype(jnp.int32)
    ints_ref[8:16] = extra.astype(jnp.int32)
    reals_ref[0:8] = near * live
    reals_ref[8:16] = far * live
    reals_ref[16:24] = jnp.where(at == 0, across - col, width * (scale / 7.0))


def make_plan(band, boxes, levels, tiles, capacity, fine_rows, coarse_rows, stride):
    smem = pl.BlockSpec(memory_space=pltpu.SMEM)
    vmem = pl.BlockSpec(memory_space=pltpu.VMEM)

    def kernel(*refs):
        plan_kernel(*refs, shape=(tiles, capacity, fine_rows, coarse_rows, stride))

    return pl.pallas_call(
        kernel,
        out_shape=(
            jax.ShapeDtypeStruct(levels.shape, jnp.int32),
            jax.ShapeDtypeStruct((16, capacity), jnp.int32),
            jax.ShapeDtypeStruct((24, capacity), F32),
        ),
        in_specs=[smem, vmem, vmem],
        out_specs=(vmem, vmem, vmem),
        compiler_params=pltpu.CompilerParams(vmem_limit_bytes=8 << 20),
        name="plan",
    )(band, boxes, levels)


def fill_maps(maps, fine_ref, coarse_ref, below, arrived):
    fine_rows, fine_cols, channels = fine_ref.shape
    coarse_rows, coarse_cols, _ = coarse_ref.shape
    total, pitch, _ = maps.shape
    base = fine_rows + REACH
    fine_copy = pltpu.make_async_copy(
        fine_ref, maps.at[0:fine_rows, 0:fine_cols, :], arrived.at[0]
    )
    fine_copy.start()
    maps[0:base, fine_cols:pitch, :] = jnp.zeros((base, pitch - fine_cols, channels), BF)
    margin = coarse_cols // 16 * 16
    maps[base:total, margin : margin + SPAN, :] = jnp.zeros((total - base, SPAN, channels), BF)
    maps[base : base + coarse_rows, 0:coarse_cols, :] = coarse_ref[...]
    if below is None:
        maps[fine_rows:base, 0:fine_cols, :] = jnp.zeros((REACH, fine_cols, channels), BF)
        maps[base + coarse_rows : total, 0:margin, :] = jnp.zeros((REACH, margin, channels), BF)
    else:
        maps[fine_rows:base, 0:fine_cols, :] = below[0][...]
        maps[base + coarse_rows : total, 0:coarse_cols, :] = below[1][...]
    fine_copy.wait()


def fill_cells(bin_ref, cell_ref):
    line = lax.broadcasted_iota(jnp.int32, bin_ref.shape, 0)
    lane = lax.broadcasted_iota(jnp.int32, bin_ref.shape, 1)
    bin_ref[...] = line.astype(F32) + 0.5
    cell_ref[...] = (lane % SPAN).astype(F32)


def crop_group(step, ints_ref, reals_ref, bin_ref, cell_ref, maps, parts, crops):
    channels = maps.shape[2]
    bins = parts.shape[1]
    first = step * GROUP
    for g in range(GROUP):
        slot = first + g
        col = pl.multiple_of(ints_ref[8, slot], 16)
        lines = []
        for i in range(7):
            row = ints_ref[i, slot]
            upper = maps[row, pl.ds(col, SPAN), :]
            lower = maps[row + 1, pl.ds(col, SPAN), :]
            near = jnp.full(upper.shape, reals_ref[i, slot], F32).astype(BF)
            far = jnp.full(upper.shape, reals_ref[8 + i, slot], F32).astype(BF)
            lines.append(near * upper + far * lower)
        lines.append(jnp.zeros((SPAN, channels), BF))
        stacked = jnp.concatenate(lines, axis=0)
        away = (reals_ref[16, slot] + bin_ref[...] * reals_ref[17, slot]) - cell_ref[...]
        line = jnp.maximum(0.0, 1.0 - jnp.abs(away))
        piece = lax.broadcasted_iota(jnp.int32, line.shape, 1) // SPAN
        mix = [jnp.where(piece == i, line, 0.0) for i in range(7)]
        mix = jnp.concatenate(mix, axis=0).astype(BF)
        parts[g] = jnp.dot(mix, stacked, preferred_element_type=F32)
    flat = parts.reshape(GROUP * bins, channels)
    start = pl.multiple_of(first, GROUP)
    for m in range(49):
        at = m // 7 * 8 + m % 7
        crops[m, pl.ds(start, GROUP), :] = flat[pl.ds(at, GROUP, stride=bins), :]


def inner_kernel(ints_ref, reals_ref, fine_ref, coarse_ref, crops_ref, maps, parts, bin_ref,
                 cell_ref, arrived):
    fill_cells(bin_ref, cell_ref)
    fill_maps(maps, fine_ref, coarse_ref, None, arrived)

    def body(step, carry):
        crop_group(step, ints_ref, reals_ref, bin_ref, cell_ref, maps, parts, crops_ref)
        return carry

    lax.fori_loop(0, crops_ref.shape[1] // GROUP, body, 0)


def edge_kernel(ints_ref, reals_ref, fine_ref, coarse_ref, fine_below_ref, coarse_below_ref,
                inner_ref, band_ref, *rest):
    *outs, maps, parts, bin_ref, cell_ref, arrived, crops, flipped = rest
    channels = fine_ref.shape[2]
    fill_cells(bin_ref, cell_ref)
    fill_maps(maps, fine_ref, coarse_ref, (fine_below_ref, coarse_below_ref), arrived)
    low = ints_ref[9, 0] // GROUP
    high = (ints_ref[10, 0] + (GROUP - 1)) // GROUP

    def body(step, carry):
        crop_group(step, ints_ref, reals_ref, bin_ref, cell_ref, maps, parts, crops)
        return carry

    lax.fori_loop(low, high, body, 0)
    at = lax.broadcasted_iota(jnp.int32, (crops.shape[1], channels), 0)
    redone = (at >= low * GROUP) & (at < high * GROUP)
    for m in range(49):
        block = jnp.where(redone, crops[m], inner_ref[m])
        flipped[m * channels : (m + 1) * channels, :] = block.T.astype(BF)
    share = outs[0].shape[0]
    for k, out in enumerate(outs):
        block = (band_ref[0] + k) % len(outs)
        out[...] = flipped[pl.ds(pl.multiple_of(block * share, 16), share), :]


def make_crops(ints, reals, fine, coarse, band, tiles):
    capacity = ints.shape[1]
    channels = fine.shape[2]
    total = fine.shape[0] + coarse.shape[0] + 2 * REACH
    smem = pl.BlockSpec(memory_space=pltpu.SMEM)
    vmem = pl.BlockSpec(memory_space=pltpu.VMEM)
    away = pl.BlockSpec(memory_space=pltpu.HBM)
    common = [
        pltpu.VMEM((total, 192, channels), BF),
        pltpu.VMEM((GROUP, 56, channels), F32),
        pltpu.VMEM((8, 8 * SPAN), F32),
        pltpu.VMEM((8, 8 * SPAN), F32),
        pltpu.SemaphoreType.DMA((1,)),
    ]
    every = jax.ShapeDtypeStruct((49, capacity, channels), F32)
    params = pltpu.CompilerParams(vmem_limit_bytes=24 << 20)
    inner = pl.pallas_call(
        inner_kernel,
        out_shape=every,
        in_specs=[smem, smem, away, vmem],
        out_specs=vmem,
        scratch_shapes=common,
        compiler_params=params,
        name="inner",
    )
    edge = pl.pallas_call(
        edge_kernel,
        out_shape=[jax.ShapeDtypeStruct((49 * channels // tiles, capacity), BF)] * tiles,
        in_specs=[smem, smem, away, vmem, vmem, vmem, vmem, smem],
        out_specs=[vmem] * tiles,
        scratch_shapes=common
        + [
            pltpu.VMEM(every.shape, F32),
            pltpu.VMEM((49 * channels, capacity), BF),
        ],
        compiler_params=params,
        name="edge",
    )
    early = inner(ints, reals, fine, coarse)
    return early, lambda early, fine_below, coarse_below: edge(
        ints, reals, fine, coarse, fine_below, coarse_below, early, band
    )


def pick_rows(turns, band_ref, slot_ref, recvs, joined, pick, arrived):
    count, capacity = band_ref[1], recvs[0].shape[1]
    slots = slot_ref[...]
    moves = [
        pltpu.make_async_copy(
            recv, joined.at[:, k * capacity : (k + 1) * capacity], arrived.at[k]
        )
        for k, recv in enumerate(recvs)
    ]
    for move in moves:
        move.start()
    for k, turn in enumerate(turns):
        source = (band_ref[0] + count - turn) % count
        at = lax.broadcasted_iota(jnp.int32, (capacity, slots.shape[1]), 0) + source * capacity
        pick[k * capacity : (k + 1) * capacity, :] = jnp.where(at == slots, 1.0, 0.0).astype(BF)
    for move in moves:
        move.wait()
    return jnp.dot(joined[...], pick[...], preferred_element_type=F32)


def make_gather(band, slot_id, recvs, turns):
    share, capacity = recvs[0].shape
    props = slot_id.shape[1]
    count = len(recvs)
    smem = pl.BlockSpec(memory_space=pltpu.SMEM)
    vmem = pl.BlockSpec(memory_space=pltpu.VMEM)

    def gather_kernel(band_ref, slot_ref, *rest):
        *pieces, out_ref, joined, pick, arrived = rest
        out_ref[...] = pick_rows(turns, band_ref, slot_ref, pieces, joined, pick, arrived).astype(BF)

    return pl.pallas_call(
        gather_kernel,
        out_shape=jax.ShapeDtypeStruct((share, props), BF),
        in_specs=[smem, vmem] + [pl.BlockSpec(memory_space=pl.ANY)] * count,
        out_specs=vmem,
        scratch_shapes=[
            pltpu.VMEM((share, count * capacity), BF),
            pltpu.VMEM((count * capacity, props), BF),
            pltpu.SemaphoreType.DMA((count,)),
        ],
        compiler_params=pltpu.CompilerParams(vmem_limit_bytes=16 << 20),
        name="gather",
    )(band, slot_id, *recvs)


def make_hidden(band, slot_id, weight, begun, recvs, turns):
    share, capacity = recvs[0].shape
    props = slot_id.shape[1]
    count = len(recvs)
    smem = pl.BlockSpec(memory_space=pltpu.SMEM)
    vmem = pl.BlockSpec(memory_space=pltpu.VMEM)

    def hidden_kernel(band_ref, slot_ref, weight_ref, begun_ref, *rest):
        *pieces, feats_ref, out_ref, joined, pick, arrived = rest
        late = pick_rows(turns, band_ref, slot_ref, pieces, joined, pick, arrived)
        feats_ref[...] = begun_ref[...] + late.astype(BF)
        skip = weight_ref.shape[1] - share
        out_ref[...] = jnp.dot(
            weight_ref[:, skip:], feats_ref[...], preferred_element_type=F32
        ).astype(BF)

    return pl.pallas_call(
        hidden_kernel,
        out_shape=(
            jax.ShapeDtypeStruct((share, props), BF),
            jax.ShapeDtypeStruct((weight.shape[0], props), BF),
        ),
        in_specs=[smem, vmem, vmem, vmem] + [pl.BlockSpec(memory_space=pl.ANY)] * count,
        out_specs=(vmem, vmem),
        scratch_shapes=[
            pltpu.VMEM((share, count * capacity), BF),
            pltpu.VMEM((count * capacity, props), BF),
            pltpu.SemaphoreType.DMA((count,)),
        ],
        compiler_params=pltpu.CompilerParams(vmem_limit_bytes=24 << 20),
        name="hidden",
    )(band, slot_id, weight, begun, *recvs)


def act_kernel(pieces_ref, back_ref, act_ref, pre_ref):
    hidden = jnp.sum(pieces_ref[...].astype(F32), axis=0)
    value, slope = gelu_parts(hidden)
    act_ref[...] = value.astype(BF)
    pre = (back_ref[...] * slope).astype(BF)
    for t in range(pre_ref.shape[0]):
        pre_ref[t] = pre


def make_act(pieces, back):
    vmem = pl.BlockSpec(memory_space=pltpu.VMEM)
    return pl.pallas_call(
        act_kernel,
        out_shape=(
            jax.ShapeDtypeStruct(pieces.shape[1:], BF),
            jax.ShapeDtypeStruct(pieces.shape, BF),
        ),
        in_specs=[vmem, vmem],
        out_specs=(vmem, vmem),
        compiler_params=pltpu.CompilerParams(vmem_limit_bytes=8 << 20),
        name="act",
    )(pieces, back)


def grads_kernel(core_ref, pre_ref, feats_ref, keep_ref, give_ref):
    rows = 256
    unit = keep_ref.shape[1]
    mine = core_ref[0] == 0

    def block(step, carry):
        start = pl.multiple_of(step * rows, rows)
        first = lax.dot_general(
            pre_ref[pl.ds(start, rows), :], feats_ref[...], (((1,), (1,)), ((), ())),
            preferred_element_type=F32,
        ).astype(BF)
        for n in range(rows // (2 * unit)):
            at = step * (rows // (2 * unit)) + n
            even = first[2 * n * unit : (2 * n + 1) * unit]
            odd = first[(2 * n + 1) * unit : (2 * n + 2) * unit]
            keep_ref[at] = jnp.where(mine, even, odd)
            give_ref[at] = jnp.where(mine, odd, even)
        return carry

    lax.fori_loop(0, pre_ref.shape[0] // rows, block, 0)


def make_grads(core, pre, feats, unit):
    smem = pl.BlockSpec(memory_space=pltpu.SMEM)
    vmem = pl.BlockSpec(memory_space=pltpu.VMEM)
    half = jax.ShapeDtypeStruct((pre.shape[0] // (2 * unit), unit, feats.shape[0]), BF)
    return pl.pallas_call(
        grads_kernel,
        out_shape=(half, half),
        in_specs=[smem, vmem, vmem],
        out_specs=(vmem, vmem),
        compiler_params=pltpu.CompilerParams(vmem_limit_bytes=24 << 20),
        name="grads",
    )(core, pre, feats)


def total_kernel(*refs):
    *parts, out_ref = refs
    out_ref[...] = sum(part[...].astype(F32) for part in parts).astype(BF)


def make_total(parts):
    vmem = pl.BlockSpec(memory_space=pltpu.VMEM)
    return pl.pallas_call(
        total_kernel,
        out_shape=jax.ShapeDtypeStruct(parts[0].shape, BF),
        in_specs=[vmem] * len(parts),
        out_specs=vmem,
        compiler_params=pltpu.CompilerParams(vmem_limit_bytes=4 << 20),
        name="total",
    )(*parts)


def merge_kernel(pieces_ref, second_ref, out_ref):
    lead = second_ref.shape[2]
    out_ref[:, :, 0:lead] = second_ref[...]
    out_ref[:, :, lead:] = jnp.sum(pieces_ref[...].astype(F32), axis=0).astype(BF)


def make_merge(pieces, second):
    vmem = pl.BlockSpec(memory_space=pltpu.VMEM)
    groups, unit, width = pieces.shape[1:]
    return pl.pallas_call(
        merge_kernel,
        out_shape=jax.ShapeDtypeStruct((groups, unit, width + second.shape[2]), BF),
        in_specs=[vmem, vmem],
        out_specs=vmem,
        compiler_params=pltpu.CompilerParams(vmem_limit_bytes=8 << 20),
        name="merge",
    )(pieces, second)


def finish_kernel(pieces_ref, first_ref, second_ref):
    total = jnp.sum(pieces_ref[...].astype(F32), axis=0)
    lead = second_ref.shape[1]
    second_ref[...] = total[:, :lead]
    first_ref[...] = total[:, lead:]


def make_finish(pieces, lead):
    vmem = pl.BlockSpec(memory_space=pltpu.VMEM)
    rows, width = pieces.shape[1:]
    return pl.pallas_call(
        finish_kernel,
        out_shape=(
            jax.ShapeDtypeStruct((rows, width - lead), F32),
            jax.ShapeDtypeStruct((rows, lead), F32),
        ),
        in_specs=[vmem],
        out_specs=(vmem, vmem),
        compiler_params=pltpu.CompilerParams(vmem_limit_bytes=8 << 20),
        name="finish",
    )(pieces)


def swapped(parts, axis):
    return lax.all_to_all(parts, axis, split_axis=0, concat_axis=0, tiled=True)


def per_device(sizes, proposal_boxes, level_plan, fine_map, coarse_map, first_weight,
               second_weight, upstream):
    nx, nz, nc, tile_count = sizes
    dp = ("x", "z", "core")
    dp_count = nx * nz * nc
    band = lax.axis_index("tile")
    fine = fine_map[0]
    coarse = coarse_map[0]
    up = [(i + 1, i) for i in range(tile_count - 1)]
    fine_top, coarse_top = cut_tops(fine, coarse)
    fine_below = lax.ppermute(fine_top, "tile", up)
    coarse_below = lax.ppermute(coarse_top, "tile", up)
    mine = lax.axis_index("core")
    band_at = band[None].astype(jnp.int32)
    num_props = level_plan.shape[1]
    capacity = max(num_props // 4, num_props // tile_count)
    unit = first_weight.shape[1]
    lead = second_weight.shape[0]
    upstream_rows = upstream[0]

    slot_id, ints, reals = make_plan(
        band_at, proposal_boxes[0], level_plan, tile_count, capacity, fine.shape[0],
        coarse.shape[0], 4,
    )
    early, edge = make_crops(ints, reals, fine, coarse, band_at, tile_count)
    copies = make_copies(first_weight.T, second_weight.T, dp_count)
    weights = swapped(copies, dp).reshape(-1, copies.shape[2])
    crops = edge(early, fine_below, coarse_below)
    recvs = {0: crops[0]}
    for k in range(1, tile_count):
        route = [(i, (i + k) % tile_count) for i in range(tile_count)]
        recvs[k] = lax.ppermute(crops[k], "tile", route)
    gather_at = jnp.stack([band, jnp.int32(tile_count)]).astype(jnp.int32)
    soon, late = (0, *TURNS[:4]), TURNS[4:]
    begun = make_gather(gather_at, slot_id, [recvs[k] for k in soon], soon)
    weights, begun = lax.optimization_barrier((weights, begun))
    back_grad = lax.dot_general(
        weights[:, :lead], upstream_rows, (((0,), (1,)), ((), ())), preferred_element_type=F32
    )
    back_grad, weights = lax.optimization_barrier((back_grad, weights))
    feats, partial_hidden = make_hidden(
        gather_at, slot_id, weights, begun, [recvs[k] for k in late], late
    )
    pieces = swapped(partial_hidden.reshape(tile_count, -1, num_props), "tile")
    activated, copies = make_act(pieces, back_grad)
    pre_grad = swapped(copies, "tile").reshape(-1, num_props)
    second = lax.dot_general(
        upstream_rows, activated, (((0,), (1,)), ((), ())), preferred_element_type=F32
    )
    second = second.astype(BF).reshape(nx, nz, nc, unit, -1)
    second_keep = jnp.where(mine == 0, second[:, :, 0], second[:, :, 1])
    second_give = jnp.where(mine == 0, second[:, :, 1], second[:, :, 0])
    second_got = lax.ppermute(second_give, "core", [(0, 1), (1, 0)])
    second_both = (second_keep.astype(F32) + second_got.astype(F32)).astype(BF)
    place = lax.axis_index("x")
    parts = []
    for k in range(nx):
        part = lax.dynamic_index_in_dim(second_both, (place + k) % nx, 0, keepdims=False)
        if k > 0:
            part = lax.ppermute(part, "x", [(i, (i + k) % nx) for i in range(nx)])
        parts.append(part)
    second_total = make_total(parts)
    core_at = mine[None].astype(jnp.int32)
    keep, give = make_grads(core_at, pre_grad, feats, unit)
    got = lax.ppermute(give, "core", [(0, 1), (1, 0)])
    both = (keep.astype(F32) + got.astype(F32)).astype(BF).reshape(nx, nz, unit, -1)
    total = make_merge(swapped(both, "x"), second_total)
    first_grad, second_grad = make_finish(swapped(total, "z"), lead)
    return (first_grad.T, second_grad.T)


def solution(mesh):
    tile_count = mesh.shape["tile"]
    sizes = (4, mesh.shape["dp"] // 8, 2, tile_count)
    split = Mesh(mesh.devices.reshape(sizes), ("x", "z", "core", "tile"))
    dp = ("x", "z", "core")
    placed = (
        P(dp, None, None),
        P(dp, None),
        P(dp, "tile", None, None),
        P(dp, "tile", None, None),
        P("tile", dp),
        P("tile", dp),
        P(dp, None, None),
    )

    def step(*args):
        return per_device(sizes, *args)

    return jax.shard_map(
        step,
        mesh=split,
        in_specs=placed,
        out_specs=(P("tile", dp), P("tile", dp)),
        check_vma=False,
    )
```

```python
import jax
import jax.numpy as jnp
from jax import lax
from jax.experimental import pallas as pl
from jax.experimental.pallas import tpu as pltpu
from jax.sharding import Mesh, PartitionSpec as P


REACH = 14
SPAN = 32
GROUP = 8
TURNS = (4, 7, 1, 6, 2, 5, 3)
BF = jnp.bfloat16
F32 = jnp.float32


def gelu_parts(hidden):
    factor = 0.7978845608028654
    cubic_term = 0.044715
    inner_term = factor * (hidden + cubic_term * hidden * hidden * hidden)
    tangent = jnp.tanh(inner_term)
    gelu_value = 0.5 * hidden * (1.0 + tangent)
    gelu_slope = 0.5 * (1.0 + tangent) + 0.5 * hidden * (1.0 - tangent * tangent) * factor * (
        1.0 + 3.0 * cubic_term * hidden * hidden
    )
    return (gelu_value, gelu_slope)


def top_kernel(fine_ref, coarse_ref, fine_top_ref, coarse_top_ref, arrived):
    moves = [
        pltpu.make_async_copy(fine_ref.at[0:REACH], fine_top_ref, arrived.at[0]),
        pltpu.make_async_copy(coarse_ref.at[0:REACH], coarse_top_ref, arrived.at[1]),
    ]
    for move in moves:
        move.start()
    for move in moves:
        move.wait()


def cut_tops(fine, coarse):
    away = pl.BlockSpec(memory_space=pltpu.HBM)
    return pl.pallas_call(
        top_kernel,
        out_shape=(
            jax.ShapeDtypeStruct((REACH, *fine.shape[1:]), BF),
            jax.ShapeDtypeStruct((REACH, *coarse.shape[1:]), BF),
        ),
        in_specs=[away, away],
        out_specs=(pl.BlockSpec(memory_space=pltpu.VMEM), pl.BlockSpec(memory_space=pltpu.VMEM)),
        scratch_shapes=[pltpu.SemaphoreType.DMA((2,))],
        compiler_params=pltpu.CompilerParams(vmem_limit_bytes=60 << 20),
        name="tops",
    )(fine, coarse)


def copies_kernel(first_ref, second_ref, out_ref):
    lead = second_ref.shape[1]
    first = first_ref[...]
    second = second_ref[...]

    def body(i, carry):
        out_ref[i, :, 0:lead] = second
        out_ref[i, :, lead:] = first
        return carry

    lax.fori_loop(0, out_ref.shape[0], body, 0)


def make_copies(first, second, count):
    vmem = pl.BlockSpec(memory_space=pltpu.VMEM)
    width = first.shape[1] + second.shape[1]
    return pl.pallas_call(
        copies_kernel,
        out_shape=jax.ShapeDtypeStruct((count, first.shape[0], width), BF),
        in_specs=[vmem, vmem],
        out_specs=vmem,
        compiler_params=pltpu.CompilerParams(vmem_limit_bytes=60 << 20),
        name="copies",
    )(first, second)


def plan_kernel(band_ref, box_ref, level_ref, slot_ref, ints_ref, reals_ref, *, shape):
    tiles, capacity, fine_rows, coarse_rows, stride = shape
    props = level_ref.shape[1]
    band = band_ref[0]
    top, left, height, width = (box_ref[i : i + 1, :] for i in range(4))
    level = level_ref[...]
    rows_px = stride * fine_rows
    owner = jnp.zeros_like(top)
    for b in range(1, tiles):
        owner = owner + jnp.where(top >= b * rows_px, 1, 0)
    down = (top - owner * rows_px).astype(F32)
    scale = jnp.where(level == 0, 1.0 / stride, 0.5 / stride)
    last = down * scale + 6.5 * height.astype(F32) * (scale / 7.0)
    limit = jnp.where(level == 0, float(fine_rows), float(coarse_rows))
    crosses = jnp.where(last >= limit - 1.01, 1.0, 0.0)
    inside = lax.broadcasted_iota(jnp.int32, (tiles, props), 0) == owner
    late = jnp.where(inside, crosses, 0.0)
    early = jnp.where(inside, 1.0 - crosses, 0.0)
    upto = lax.broadcasted_iota(jnp.int32, (props, props), 0) <= lax.broadcasted_iota(
        jnp.int32, (props, props), 1
    )
    upto = jnp.where(upto, 1.0, 0.0).astype(BF)
    both = jnp.concatenate([early, late], axis=0).astype(BF)
    order = jnp.dot(both, upto, preferred_element_type=F32)
    first = jnp.sum(early, axis=1, keepdims=True)
    every = first + jnp.sum(late, axis=1, keepdims=True)
    rank = early * (order[:tiles] - 1.0) + late * (order[tiles:] + first - 1.0)
    rank = jnp.sum(rank, axis=0, keepdims=True).astype(jnp.int32)
    slot = owner * capacity + rank
    slot_ref[...] = slot
    here = lax.broadcasted_iota(jnp.int32, (capacity, props), 0) + band * capacity == slot
    here = jnp.where(here, 1.0, 0.0).astype(BF)
    fields = jnp.concatenate(
        [
            down,
            (left // 8).astype(F32),
            (left % 8).astype(F32),
            height.astype(F32),
            width.astype(F32),
            level.astype(F32),
            jnp.ones_like(down),
            jnp.zeros_like(down),
        ],
        axis=0,
    ).astype(BF)
    fields = jnp.concatenate([fields, jnp.zeros_like(fields)], axis=0)
    taken = lax.dot_general(fields, here, (((1,), (1,)), ((), ())), preferred_element_type=F32)
    down, left_high, left_low, height, width, level, live = (taken[i : i + 1] for i in range(7))
    scale = jnp.where(level > 0.5, 0.5 / stride, 1.0 / stride)
    step = lax.broadcasted_iota(jnp.int32, (8, capacity), 0).astype(F32) + 0.5
    point = down * scale + step * (height * (scale / 7.0))
    whole = jnp.floor(point)
    near = jnp.maximum(0.0, 1.0 - (point - whole)).astype(BF).astype(F32)
    far = jnp.maximum(0.0, 1.0 - (whole + 1.0 - point)).astype(BF).astype(F32)
    most = jnp.where(level > 0.5, float(coarse_rows), float(fine_rows)) + (REACH - 2.0)
    whole = jnp.clip(whole, 0.0, most) + jnp.where(level > 0.5, fine_rows + float(REACH), 0.0)
    across = (left_high * 8.0 + left_low) * scale
    col = jnp.floor(across * 0.0625) * 16.0
    own = lax.broadcasted_iota(jnp.int32, (tiles, 1), 0) == band
    early_count = jnp.sum(jnp.where(own, first, 0.0), axis=0, keepdims=True)
    every_count = jnp.sum(jnp.where(own, every, 0.0), axis=0, keepdims=True)
    at = lax.broadcasted_iota(jnp.int32, (8, capacity), 0)
    extra = jnp.where(at == 0, col, jnp.where(at == 1, early_count, every_count))
    ints_ref[0:8] = whole.astype(jnp.int32)
    ints_ref[8:16] = extra.astype(jnp.int32)
    reals_ref[0:8] = near * live
    reals_ref[8:16] = far * live
    reals_ref[16:24] = jnp.where(at == 0, across - col, width * (scale / 7.0))


def make_plan(band, boxes, levels, tiles, capacity, fine_rows, coarse_rows, stride):
    smem = pl.BlockSpec(memory_space=pltpu.SMEM)
    vmem = pl.BlockSpec(memory_space=pltpu.VMEM)

    def kernel(*refs):
        plan_kernel(*refs, shape=(tiles, capacity, fine_rows, coarse_rows, stride))

    return pl.pallas_call(
        kernel,
        out_shape=(
            jax.ShapeDtypeStruct(levels.shape, jnp.int32),
            jax.ShapeDtypeStruct((16, capacity), jnp.int32),
            jax.ShapeDtypeStruct((24, capacity), F32),
        ),
        in_specs=[smem, vmem, vmem],
        out_specs=(vmem, vmem, vmem),
        compiler_params=pltpu.CompilerParams(vmem_limit_bytes=8 << 20),
        name="plan",
    )(band, boxes, levels)


def fill_maps(maps, fine_ref, coarse_ref, below, arrived):
    fine_rows, fine_cols, channels = fine_ref.shape
    coarse_rows, coarse_cols, _ = coarse_ref.shape
    total, pitch, _ = maps.shape
    base = fine_rows + REACH
    fine_copy = pltpu.make_async_copy(
        fine_ref, maps.at[0:fine_rows, 0:fine_cols, :], arrived.at[0]
    )
    fine_copy.start()
    maps[0:base, fine_cols:pitch, :] = jnp.zeros((base, pitch - fine_cols, channels), BF)
    margin = coarse_cols // 16 * 16
    maps[base:total, margin : margin + SPAN, :] = jnp.zeros((total - base, SPAN, channels), BF)
    maps[base : base + coarse_rows, 0:coarse_cols, :] = coarse_ref[...]
    if below is None:
        maps[fine_rows:base, 0:fine_cols, :] = jnp.zeros((REACH, fine_cols, channels), BF)
        maps[base + coarse_rows : total, 0:margin, :] = jnp.zeros((REACH, margin, channels), BF)
    else:
        maps[fine_rows:base, 0:fine_cols, :] = below[0][...]
        maps[base + coarse_rows : total, 0:coarse_cols, :] = below[1][...]
    fine_copy.wait()


def fill_cells(bin_ref, cell_ref):
    line = lax.broadcasted_iota(jnp.int32, bin_ref.shape, 0)
    lane = lax.broadcasted_iota(jnp.int32, bin_ref.shape, 1)
    bin_ref[...] = line.astype(F32) + 0.5
    cell_ref[...] = (lane % SPAN).astype(F32)


def crop_group(step, ints_ref, reals_ref, bin_ref, cell_ref, maps, parts, crops):
    channels = maps.shape[2]
    bins = parts.shape[1]
    first = step * GROUP
    for g in range(GROUP):
        slot = first + g
        col = pl.multiple_of(ints_ref[8, slot], 16)
        lines = []
        for i in range(7):
            row = ints_ref[i, slot]
            upper = maps[row, pl.ds(col, SPAN), :]
            lower = maps[row + 1, pl.ds(col, SPAN), :]
            near = jnp.full(upper.shape, reals_ref[i, slot], F32).astype(BF)
            far = jnp.full(upper.shape, reals_ref[8 + i, slot], F32).astype(BF)
            lines.append(near * upper + far * lower)
        lines.append(jnp.zeros((SPAN, channels), BF))
        stacked = jnp.concatenate(lines, axis=0)
        away = (reals_ref[16, slot] + bin_ref[...] * reals_ref[17, slot]) - cell_ref[...]
        line = jnp.maximum(0.0, 1.0 - jnp.abs(away))
        piece = lax.broadcasted_iota(jnp.int32, line.shape, 1) // SPAN
        mix = [jnp.where(piece == i, line, 0.0) for i in range(7)]
        mix = jnp.concatenate(mix, axis=0).astype(BF)
        parts[g] = jnp.dot(mix, stacked, preferred_element_type=F32)
    flat = parts.reshape(GROUP * bins, channels)
    start = pl.multiple_of(first, GROUP)
    for m in range(49):
        at = m // 7 * 8 + m % 7
        crops[m, pl.ds(start, GROUP), :] = flat[pl.ds(at, GROUP, stride=bins), :]


def inner_kernel(ints_ref, reals_ref, fine_ref, coarse_ref, crops_ref, maps, parts, bin_ref,
                 cell_ref, arrived):
    fill_cells(bin_ref, cell_ref)
    fill_maps(maps, fine_ref, coarse_ref, None, arrived)

    def body(step, carry):
        crop_group(step, ints_ref, reals_ref, bin_ref, cell_ref, maps, parts, crops_ref)
        return carry

    lax.fori_loop(0, crops_ref.shape[1] // GROUP, body, 0)


def edge_kernel(ints_ref, reals_ref, fine_ref, coarse_ref, fine_below_ref, coarse_below_ref,
                inner_ref, band_ref, *rest):
    *outs, maps, parts, bin_ref, cell_ref, arrived, crops, flipped = rest
    channels = fine_ref.shape[2]
    fill_cells(bin_ref, cell_ref)
    fill_maps(maps, fine_ref, coarse_ref, (fine_below_ref, coarse_below_ref), arrived)
    low = ints_ref[9, 0] // GROUP
    high = (ints_ref[10, 0] + (GROUP - 1)) // GROUP

    def body(step, carry):
        crop_group(step, ints_ref, reals_ref, bin_ref, cell_ref, maps, parts, crops)
        return carry

    lax.fori_loop(low, high, body, 0)
    at = lax.broadcasted_iota(jnp.int32, (crops.shape[1], channels), 0)
    redone = (at >= low * GROUP) & (at < high * GROUP)
    for m in range(49):
        block = jnp.where(redone, crops[m], inner_ref[m])
        flipped[m * channels : (m + 1) * channels, :] = block.T.astype(BF)
    share = outs[0].shape[0]
    for k, out in enumerate(outs):
        block = (band_ref[0] + k) % len(outs)
        out[...] = flipped[pl.ds(pl.multiple_of(block * share, 16), share), :]


def make_crops(ints, reals, fine, coarse, band, tiles):
    capacity = ints.shape[1]
    channels = fine.shape[2]
    total = fine.shape[0] + coarse.shape[0] + 2 * REACH
    smem = pl.BlockSpec(memory_space=pltpu.SMEM)
    vmem = pl.BlockSpec(memory_space=pltpu.VMEM)
    away = pl.BlockSpec(memory_space=pltpu.HBM)
    common = [
        pltpu.VMEM((total, 192, channels), BF),
        pltpu.VMEM((GROUP, 56, channels), F32),
        pltpu.VMEM((8, 8 * SPAN), F32),
        pltpu.VMEM((8, 8 * SPAN), F32),
        pltpu.SemaphoreType.DMA((1,)),
    ]
    every = jax.ShapeDtypeStruct((49, capacity, channels), F32)
    params = pltpu.CompilerParams(vmem_limit_bytes=24 << 20)
    inner = pl.pallas_call(
        inner_kernel,
        out_shape=every,
        in_specs=[smem, smem, away, vmem],
        out_specs=vmem,
        scratch_shapes=common,
        compiler_params=params,
        name="inner",
    )
    edge = pl.pallas_call(
        edge_kernel,
        out_shape=[jax.ShapeDtypeStruct((49 * channels // tiles, capacity), BF)] * tiles,
        in_specs=[smem, smem, away, vmem, vmem, vmem, vmem, smem],
        out_specs=[vmem] * tiles,
        scratch_shapes=common
        + [
            pltpu.VMEM(every.shape, F32),
            pltpu.VMEM((49 * channels, capacity), BF),
        ],
        compiler_params=params,
        name="edge",
    )
    early = inner(ints, reals, fine, coarse)
    return early, lambda early, fine_below, coarse_below: edge(
        ints, reals, fine, coarse, fine_below, coarse_below, early, band
    )


def pick_rows(turns, band_ref, slot_ref, recvs, joined, pick, arrived):
    count, capacity = band_ref[1], recvs[0].shape[1]
    slots = slot_ref[...]
    moves = [
        pltpu.make_async_copy(
            recv, joined.at[:, k * capacity : (k + 1) * capacity], arrived.at[k]
        )
        for k, recv in enumerate(recvs)
    ]
    for move in moves:
        move.start()
    for k, turn in enumerate(turns):
        source = (band_ref[0] + count - turn) % count
        at = lax.broadcasted_iota(jnp.int32, (capacity, slots.shape[1]), 0) + source * capacity
        pick[k * capacity : (k + 1) * capacity, :] = jnp.where(at == slots, 1.0, 0.0).astype(BF)
    for move in moves:
        move.wait()
    return jnp.dot(joined[...], pick[...], preferred_element_type=F32)


def make_gather(band, slot_id, recvs, turns):
    share, capacity = recvs[0].shape
    props = slot_id.shape[1]
    count = len(recvs)
    smem = pl.BlockSpec(memory_space=pltpu.SMEM)
    vmem = pl.BlockSpec(memory_space=pltpu.VMEM)

    def gather_kernel(band_ref, slot_ref, *rest):
        *pieces, out_ref, joined, pick, arrived = rest
        out_ref[...] = pick_rows(turns, band_ref, slot_ref, pieces, joined, pick, arrived).astype(BF)

    return pl.pallas_call(
        gather_kernel,
        out_shape=jax.ShapeDtypeStruct((share, props), BF),
        in_specs=[smem, vmem] + [pl.BlockSpec(memory_space=pl.ANY)] * count,
        out_specs=vmem,
        scratch_shapes=[
            pltpu.VMEM((share, count * capacity), BF),
            pltpu.VMEM((count * capacity, props), BF),
            pltpu.SemaphoreType.DMA((count,)),
        ],
        compiler_params=pltpu.CompilerParams(vmem_limit_bytes=16 << 20),
        name="gather",
    )(band, slot_id, *recvs)


def make_hidden(band, slot_id, weight, begun, recvs, turns):
    share, capacity = recvs[0].shape
    props = slot_id.shape[1]
    count = len(recvs)
    smem = pl.BlockSpec(memory_space=pltpu.SMEM)
    vmem = pl.BlockSpec(memory_space=pltpu.VMEM)

    def hidden_kernel(band_ref, slot_ref, weight_ref, begun_ref, *rest):
        *pieces, feats_ref, out_ref, joined, pick, arrived = rest
        late = pick_rows(turns, band_ref, slot_ref, pieces, joined, pick, arrived)
        feats_ref[...] = begun_ref[...] + late.astype(BF)
        skip = weight_ref.shape[1] - share
        out_ref[...] = jnp.dot(
            weight_ref[:, skip:], feats_ref[...], preferred_element_type=F32
        ).astype(BF)

    return pl.pallas_call(
        hidden_kernel,
        out_shape=(
            jax.ShapeDtypeStruct((share, props), BF),
            jax.ShapeDtypeStruct((weight.shape[0], props), BF),
        ),
        in_specs=[smem, vmem, vmem, vmem] + [pl.BlockSpec(memory_space=pl.ANY)] * count,
        out_specs=(vmem, vmem),
        scratch_shapes=[
            pltpu.VMEM((share, count * capacity), BF),
            pltpu.VMEM((count * capacity, props), BF),
            pltpu.SemaphoreType.DMA((count,)),
        ],
        compiler_params=pltpu.CompilerParams(vmem_limit_bytes=24 << 20),
        name="hidden",
    )(band, slot_id, weight, begun, *recvs)


def act_kernel(pieces_ref, back_ref, act_ref, pre_ref):
    hidden = jnp.sum(pieces_ref[...].astype(F32), axis=0)
    value, slope = gelu_parts(hidden)
    act_ref[...] = value.astype(BF)
    pre = (back_ref[...] * slope).astype(BF)
    for t in range(pre_ref.shape[0]):
        pre_ref[t] = pre


def make_act(pieces, back):
    vmem = pl.BlockSpec(memory_space=pltpu.VMEM)
    return pl.pallas_call(
        act_kernel,
        out_shape=(
            jax.ShapeDtypeStruct(pieces.shape[1:], BF),
            jax.ShapeDtypeStruct(pieces.shape, BF),
        ),
        in_specs=[vmem, vmem],
        out_specs=(vmem, vmem),
        compiler_params=pltpu.CompilerParams(vmem_limit_bytes=8 << 20),
        name="act",
    )(pieces, back)


def grads_kernel(core_ref, pre_ref, feats_ref, keep_ref, give_ref):
    rows = 256
    unit = keep_ref.shape[1]
    mine = core_ref[0] == 0

    def block(step, carry):
        start = pl.multiple_of(step * rows, rows)
        first = lax.dot_general(
            pre_ref[pl.ds(start, rows), :], feats_ref[...], (((1,), (1,)), ((), ())),
            preferred_element_type=F32,
        ).astype(BF)
        for n in range(rows // (2 * unit)):
            at = step * (rows // (2 * unit)) + n
            even = first[2 * n * unit : (2 * n + 1) * unit]
            odd = first[(2 * n + 1) * unit : (2 * n + 2) * unit]
            keep_ref[at] = jnp.where(mine, even, odd)
            give_ref[at] = jnp.where(mine, odd, even)
        return carry

    lax.fori_loop(0, pre_ref.shape[0] // rows, block, 0)


def make_grads(core, pre, feats, unit):
    smem = pl.BlockSpec(memory_space=pltpu.SMEM)
    vmem = pl.BlockSpec(memory_space=pltpu.VMEM)
    half = jax.ShapeDtypeStruct((pre.shape[0] // (2 * unit), unit, feats.shape[0]), BF)
    return pl.pallas_call(
        grads_kernel,
        out_shape=(half, half),
        in_specs=[smem, vmem, vmem],
        out_specs=(vmem, vmem),
        compiler_params=pltpu.CompilerParams(vmem_limit_bytes=24 << 20),
        name="grads",
    )(core, pre, feats)


def total_kernel(*refs):
    *parts, out_ref = refs
    out_ref[...] = sum(part[...].astype(F32) for part in parts).astype(BF)


def make_total(parts):
    vmem = pl.BlockSpec(memory_space=pltpu.VMEM)
    return pl.pallas_call(
        total_kernel,
        out_shape=jax.ShapeDtypeStruct(parts[0].shape, BF),
        in_specs=[vmem] * len(parts),
        out_specs=vmem,
        compiler_params=pltpu.CompilerParams(vmem_limit_bytes=4 << 20),
        name="total",
    )(*parts)


def merge_kernel(pieces_ref, second_ref, out_ref):
    lead = second_ref.shape[2]
    out_ref[:, :, 0:lead] = second_ref[...]
    out_ref[:, :, lead:] = jnp.sum(pieces_ref[...].astype(F32), axis=0).astype(BF)


def make_merge(pieces, second):
    vmem = pl.BlockSpec(memory_space=pltpu.VMEM)
    groups, unit, width = pieces.shape[1:]
    return pl.pallas_call(
        merge_kernel,
        out_shape=jax.ShapeDtypeStruct((groups, unit, width + second.shape[2]), BF),
        in_specs=[vmem, vmem],
        out_specs=vmem,
        compiler_params=pltpu.CompilerParams(vmem_limit_bytes=8 << 20),
        name="merge",
    )(pieces, second)


def finish_kernel(pieces_ref, first_ref, second_ref):
    total = jnp.sum(pieces_ref[...].astype(F32), axis=0)
    lead = second_ref.shape[1]
    second_ref[...] = total[:, :lead]
    first_ref[...] = total[:, lead:]


def make_finish(pieces, lead):
    vmem = pl.BlockSpec(memory_space=pltpu.VMEM)
    rows, width = pieces.shape[1:]
    return pl.pallas_call(
        finish_kernel,
        out_shape=(
            jax.ShapeDtypeStruct((rows, width - lead), F32),
            jax.ShapeDtypeStruct((rows, lead), F32),
        ),
        in_specs=[vmem],
        out_specs=(vmem, vmem),
        compiler_params=pltpu.CompilerParams(vmem_limit_bytes=8 << 20),
        name="finish",
    )(pieces)


def swapped(parts, axis):
    return lax.all_to_all(parts, axis, split_axis=0, concat_axis=0, tiled=True)


def per_device(sizes, proposal_boxes, level_plan, fine_map, coarse_map, first_weight,
               second_weight, upstream):
    nx, nz, nc, tile_count = sizes
    dp = ("x", "z", "core")
    dp_count = nx * nz * nc
    band = lax.axis_index("tile")
    fine = fine_map[0]
    coarse = coarse_map[0]
    up = [(i + 1, i) for i in range(tile_count - 1)]
    fine_top, coarse_top = cut_tops(fine, coarse)
    fine_below = lax.ppermute(fine_top, "tile", up)
    coarse_below = lax.ppermute(coarse_top, "tile", up)
    mine = lax.axis_index("core")
    band_at = band[None].astype(jnp.int32)
    num_props = level_plan.shape[1]
    capacity = max(num_props // 4, num_props // tile_count)
    unit = first_weight.shape[1]
    lead = second_weight.shape[0]
    upstream_rows = upstream[0]

    slot_id, ints, reals = make_plan(
        band_at, proposal_boxes[0], level_plan, tile_count, capacity, fine.shape[0],
        coarse.shape[0], 4,
    )
    early, edge = make_crops(ints, reals, fine, coarse, band_at, tile_count)
    copies = make_copies(first_weight.T, second_weight.T, dp_count)
    weights = swapped(copies, dp).reshape(-1, copies.shape[2])
    crops = edge(early, fine_below, coarse_below)
    recvs = {0: crops[0]}
    for k in range(1, tile_count):
        route = [(i, (i + k) % tile_count) for i in range(tile_count)]
        recvs[k] = lax.ppermute(crops[k], "tile", route)
    gather_at = jnp.stack([band, jnp.int32(tile_count)]).astype(jnp.int32)
    soon, late = (0, *TURNS[:4]), TURNS[4:]
    begun = make_gather(gather_at, slot_id, [recvs[k] for k in soon], soon)
    weights, begun = lax.optimization_barrier((weights, begun))
    back_grad = lax.dot_general(
        weights[:, :lead], upstream_rows, (((0,), (1,)), ((), ())), preferred_element_type=F32
    )
    back_grad, weights = lax.optimization_barrier((back_grad, weights))
    feats, partial_hidden = make_hidden(
        gather_at, slot_id, weights, begun, [recvs[k] for k in late], late
    )
    pieces = swapped(partial_hidden.reshape(tile_count, -1, num_props), "tile")
    activated, copies = make_act(pieces, back_grad)
    pre_grad = swapped(copies, "tile").reshape(-1, num_props)
    second = lax.dot_general(
        upstream_rows, activated, (((0,), (1,)), ((), ())), preferred_element_type=F32
    )
    second = second.astype(BF).reshape(nx, nz, nc, unit, -1)
    second_keep = jnp.where(mine == 0, second[:, :, 0], second[:, :, 1])
    second_give = jnp.where(mine == 0, second[:, :, 1], second[:, :, 0])
    second_got = lax.ppermute(second_give, "core", [(0, 1), (1, 0)])
    second_both = (second_keep.astype(F32) + second_got.astype(F32)).astype(BF)
    place = lax.axis_index("x")
    parts = []
    for k in range(nx):
        part = lax.dynamic_index_in_dim(second_both, (place + k) % nx, 0, keepdims=False)
        if k > 0:
            part = lax.ppermute(part, "x", [(i, (i + k) % nx) for i in range(nx)])
        parts.append(part)
    second_total = make_total(parts)
    core_at = mine[None].astype(jnp.int32)
    keep, give = make_grads(core_at, pre_grad, feats, unit)
    got = lax.ppermute(give, "core", [(0, 1), (1, 0)])
    both = (keep.astype(F32) + got.astype(F32)).astype(BF).reshape(nx, nz, unit, -1)
    total = make_merge(swapped(both, "x"), second_total)
    first_grad, second_grad = make_finish(swapped(total, "z"), lead)
    return (first_grad.T, second_grad.T)


def solution(mesh):
    tile_count = mesh.shape["tile"]
    sizes = (4, mesh.shape["dp"] // 8, 2, tile_count)
    split = Mesh(mesh.devices.reshape(sizes), ("x", "z", "core", "tile"))
    dp = ("x", "z", "core")
    placed = (
        P(dp, None, None),
        P(dp, None),
        P(dp, "tile", None, None),
        P(dp, "tile", None, None),
        P("tile", dp),
        P("tile", dp),
        P(dp, None, None),
    )

    def step(*args):
        return per_device(sizes, *args)

    return jax.shard_map(
        step,
        mesh=split,
        in_specs=placed,
        out_specs=(P("tile", dp), P("tile", dp)),
        check_vma=False,
    )
```
